32 devices in a mesh: row: 4 (over y, x), col: 8 (over z, core).
Axes of the slice: x: 2, y: 2, z: 4, core: 2. Of those that a mesh axis runs over, the one named last changes fastest.
Arguments:
- features: bfloat16 [32, 512, 768], P('row', 'col'), may hold values from -6 to 6
- norm_scale: float32 [768], replicated, may hold values from 0.5 to 1.5
- norm_shift: float32 [768], replicated, may hold values from -3 to 3
- expand_weight: bfloat16 [768, 3072], replicated, may hold values from -0.21875 to 0.21875
- expand_bias: float32 [3072], replicated, may hold values from -3 to 3
- depth_kernel: float32 [3, 3, 3072], replicated, may hold values from -2 to 2
- depth_bias: float32 [3072], replicated, may hold values from -3 to 3
- project_weight: bfloat16 [3072, 768], replicated, may hold values from -0.109375 to 0.109375
- project_bias: float32 [768], replicated, may hold values from -2 to 2
- attn_gain: float32 [768], replicated, may hold values from 0.25 to 1.75
- attn_shift: float32 [768], replicated, may hold values from -2 to 2
- qkv_weight: bfloat16 [768, 2304], replicated, may hold values from -0.21875 to 0.21875
- qkv_bias: float32 [2304], replicated, may hold values from -2 to 2
- out_weight: bfloat16 [768, 768], replicated, may hold values from -0.21875 to 0.21875
- out_bias: float32 [768], replicated, may hold values from -2 to 2
Outputs:
- output: bfloat16 [32, 512, 768], P('row', 'col')
The draws below stay inside these ranges and needn't reach their ends.
All inputs are finite; a program needn't handle non-finite values.
Results may differ from the reference program's by a relative error of at most 0.006.
Values may be sent and summed in bfloat16 or wider, within the bound.
No kernel may reach another device: no remote copies, remote signals or barrier semaphores. Data moves between devices by JAX's collectives and lax.ppermute only.
A program may use at most 192 MiB of HBM per device.

```python
import math
import jax
import jax.numpy as jnp
from jax import lax

C = 768
HEADS = 24
HEAD_DIM = 32
EXPAND = 3072
GRID = 8
H = 32
W = 512


def block_levels(stream_key, dims, cuts, smallest, high):
    def one(position, parts):
        draws = jax.random.uniform(jax.random.fold_in(jax.random.fold_in(stream_key, 6), position), (parts,), jnp.float32, smallest / len(cuts), high / len(cuts))
        return jnp.repeat(jnp.exp(draws), dims[position] // parts).reshape((-1,) + (1,) * (len(dims) - position - 1))

    gain = one(*cuts[0])
    for cut in cuts[1:]:
        gain = gain * one(*cut)
    return gain


def gaussian(rng, shape, scale, limit, pieces=(), kind=jnp.bfloat16):
    factor_of = block_levels(rng, shape, pieces, -0.22, 0.18) if pieces else 1.0
    values = jax.random.normal(rng, shape, jnp.float32) * scale * factor_of
    return jnp.minimum(jnp.maximum(values, -limit), limit).astype(kind)


def setup_inputs(seed: int = 0) -> dict:
    seeds = jax.random.split(jax.random.key(seed), 16)
    return {
        "features": gaussian(seeds[0], (H, W, C), 1.0, 6.0, ((0, 4), (1, 8))),
        "norm_scale": jnp.clip(1.0 + 0.1 * jax.random.normal(seeds[1], (C,), jnp.float32), 0.5, 1.5),
        "norm_shift": gaussian(seeds[2], (C,), 0.5, 3.0, (), jnp.float32),
        "expand_weight": gaussian(seeds[3], (C, EXPAND), C ** -0.5, 0.21875),
        "expand_bias": gaussian(seeds[4], (EXPAND,), 0.5, 3.0, (), jnp.float32),
        "depth_kernel": gaussian(seeds[5], (3, 3, EXPAND), 9 ** -0.5, 2.0, (), jnp.float32),
        "depth_bias": gaussian(seeds[6], (EXPAND,), 0.5, 3.0, (), jnp.float32),
        "project_weight": gaussian(seeds[7], (EXPAND, C), EXPAND ** -0.5, 0.109375),
        "project_bias": gaussian(seeds[8], (C,), 0.3, 2.0, (), jnp.float32),
        "attn_gain": jnp.clip(1.0 + 0.15 * jax.random.normal(seeds[9], (C,), jnp.float32), 0.25, 1.75),
        "attn_shift": gaussian(seeds[10], (C,), 0.3, 2.0, (), jnp.float32),
        "qkv_weight": gaussian(seeds[11], (C, 3 * C), C ** -0.5, 0.21875),
        "qkv_bias": gaussian(seeds[12], (3 * C,), 0.3, 2.0, (), jnp.float32),
        "out_weight": gaussian(seeds[13], (C, C), C ** -0.5, 0.21875),
        "out_bias": gaussian(seeds[14], (C,), 0.3, 2.0, (), jnp.float32),
    }


def layer_norm(values, scale_vec, shift_vec):
    widened = values.astype(jnp.float32)
    center = widened - lax.optimization_barrier(jnp.mean(widened, axis=-1, keepdims=True))
    spread = lax.optimization_barrier(jnp.mean(center * center, axis=-1, keepdims=True))
    return (center * lax.rsqrt(spread + 1e-06) * scale_vec + shift_vec).astype(jnp.bfloat16)

def attend(tokens_in, pattern, qkv_weight, qkv_bias, out_weight, out_bias):
    channels = tokens_in.shape[-1]
    leading = tokens_in.shape[:-1]
    projected = jnp.dot(tokens_in.reshape(-1, channels), qkv_weight, preferred_element_type=jnp.float32) + qkv_bias
    projected = projected.astype(jnp.bfloat16).reshape(leading + (3, HEADS, HEAD_DIM))
    query_part = projected[..., 0, :, :].astype(jnp.float32)
    key_part = projected[..., 1, :, :].astype(jnp.float32)
    value_part = projected[..., 2, :, :].astype(jnp.float32)
    renamed = {'i': 'm', 'j': 'n', 'k': 'o', 'l': 'p'}
    token_letters = 'ijkl'
    key_pattern = ''.join((renamed.get(letter, letter) for letter in pattern))
    groups = ''.join((letter for letter in pattern if letter not in token_letters))
    query_tokens = ''.join((letter for letter in pattern if letter in token_letters))
    key_tokens = ''.join((renamed[letter] for letter in query_tokens))
    score_form = groups + 'h' + query_tokens + key_tokens
    scores = jnp.einsum(pattern + 'hd,' + key_pattern + 'hd->' + score_form, query_part, key_part) * (1.0 / math.sqrt(HEAD_DIM))
    weights = jnp.exp(scores)
    total = lax.optimization_barrier(jnp.sum(weights, axis=tuple(range(-len(key_tokens), 0)), keepdims=True))
    probs = (weights / total).astype(jnp.bfloat16)
    mixed = jnp.einsum(score_form + ',' + key_pattern + 'hd->' + pattern + 'hd', probs.astype(jnp.float32), value_part)
    mixed = mixed.astype(jnp.bfloat16)
    result = jnp.dot(mixed.reshape(-1, channels), out_weight, preferred_element_type=jnp.float32) + out_bias
    return result.astype(jnp.bfloat16).reshape(tokens_in.shape)

def reference(features, norm_scale, norm_shift, expand_weight, expand_bias, depth_kernel, depth_bias, project_weight, project_bias, attn_gain, attn_shift, qkv_weight, qkv_bias, out_weight, out_bias):
    normed = (features.astype(jnp.float32) * norm_scale + norm_shift).astype(jnp.bfloat16)

    def expand_row(row_in):
        return jax.nn.gelu(jnp.dot(row_in, expand_weight, preferred_element_type=jnp.float32) + expand_bias).astype(jnp.bfloat16)
    hidden = lax.map(expand_row, normed)
    padded = jnp.pad(hidden, ((1, 1), (1, 1), (0, 0)))

    def convolve_row(pair):
        row_index, row_in = pair
        window = lax.dynamic_slice_in_dim(padded, row_index, 3, 0)
        summed = jnp.zeros((W, EXPAND), jnp.float32)
        for row_off in range(3):
            for col_off in range(3):
                summed = summed + window[row_off, col_off:col_off + W].astype(jnp.float32) * depth_kernel[row_off, col_off]
        depthwise = jax.nn.gelu(summed + depth_bias).astype(jnp.bfloat16)
        projected = jnp.dot(depthwise, project_weight, preferred_element_type=jnp.float32) + project_bias
        return (row_in.astype(jnp.float32) + projected).astype(jnp.bfloat16)
    after_conv = lax.map(convolve_row, (jnp.arange(H, dtype=jnp.int32), features))
    attn_in = layer_norm(after_conv, attn_gain, attn_shift)
    stride_rows = H // GRID
    stride_cols = W // GRID
    split_view = attn_in.reshape(GRID, stride_rows, GRID, stride_cols, C).transpose(1, 0, 2, 3, 4)

    def attend_slice(piece):
        return attend(piece, 'jlv', qkv_weight, qkv_bias, out_weight, out_bias)
    answered = lax.map(attend_slice, split_view)
    attended = answered.transpose(1, 0, 2, 3, 4).reshape(H, W, C)
    return (after_conv.astype(jnp.float32) + attended.astype(jnp.float32)).astype(jnp.bfloat16)
```

```python
import functools
import math

import jax
import jax.numpy as jnp
import numpy as np
from jax import lax
from jax.experimental import pallas as pl
from jax.experimental.pallas import tpu as pltpu
from jax.sharding import PartitionSpec as P

HEADS = 24
HEAD_DIM = 32
GRID = 8
LANES = 128
PACK = LANES // HEAD_DIM


def extended(cells, sides, width):
    for axis, dim in sides:
        count = lax.axis_size(axis)
        ends = count - 1
        head = lax.slice_in_dim(cells, 0, width, axis=dim)
        tail = lax.slice_in_dim(cells, cells.shape[dim] - width, cells.shape[dim], axis=dim)
        cells = jnp.concatenate(
            [
                lax.ppermute(tail, axis, [(i, (i + 1) % count) for i in range(ends)]),
                cells,
                lax.ppermute(head, axis, [((i + 1) % count, i) for i in range(ends)]),
            ],
            axis=dim,
        )
    return cells


def expand_cells(inputs, norm_scale, norm_shift, expand_weight, expand_bias):
    normed = (inputs.astype(jnp.float32) * norm_scale + norm_shift).astype(jnp.bfloat16)
    flat_rows = normed.reshape(-1, normed.shape[-1])
    hidden = jax.nn.gelu(
        jnp.dot(flat_rows, expand_weight, preferred_element_type=jnp.float32) + expand_bias
    )
    return hidden.astype(jnp.bfloat16).reshape(inputs.shape[:-1] + (expand_weight.shape[1],))


def layer_norm(values, scale_vec, shift_vec):
    widened = values.astype(jnp.float32)
    center = widened - jnp.mean(widened, axis=-1, keepdims=True)
    spread = jnp.mean(center * center, axis=-1, keepdims=True)
    return (center * lax.rsqrt(spread + 1e-06) * scale_vec + shift_vec).astype(jnp.bfloat16)


def attend_kernel(
    group_size,
    x_ref,
    pick_ref,
    place_ref,
    qkv_weight_ref,
    qkv_bias_ref,
    out_weight_ref,
    out_bias_ref,
    o_ref,
    qkv_ref,
    mixed_ref,
    probs_ref,
):
    count, channels = x_ref.shape
    f32, bf16 = jnp.float32, jnp.bfloat16
    half = count // 2
    column = lax.broadcasted_iota(jnp.int32, (count, count), 1)
    pick = (column == pick_ref[...]).astype(f32).astype(bf16)
    x = jnp.dot(pick, x_ref[...], preferred_element_type=f32).astype(bf16)
    step = 256
    for lo in range(0, 3 * channels, step):
        cols = slice(lo, lo + step)
        part = jnp.dot(x, qkv_weight_ref[:, cols], preferred_element_type=f32)
        qkv_ref[:, cols] = (part + qkv_bias_ref[:, cols]).astype(bf16)

    wide = PACK * group_size
    lane = lax.broadcasted_iota(jnp.int32, (wide, LANES), 1) // HEAD_DIM
    row = lax.broadcasted_iota(jnp.int32, (wide, LANES), 0) // group_size
    own = (lane == row).astype(f32).astype(bf16)
    block_row = lax.broadcasted_iota(jnp.int32, (wide, wide), 0) // group_size
    block_col = lax.broadcasted_iota(jnp.int32, (wide, wide), 1) // group_size
    same = (block_row == block_col).astype(f32).astype(bf16)
    scale = math.log2(math.e) / math.sqrt(HEAD_DIM)
    top = float(jnp.finfo(bf16).max)
    chunks = channels // LANES

    def one_group(group, carry):
        rows = pl.ds(pl.multiple_of(group * group_size, group_size), group_size)
        for chunk in range(chunks):
            lo = chunk * LANES
            query = qkv_ref[rows, lo : lo + LANES]
            key = qkv_ref[rows, channels + lo : channels + lo + LANES]
            keys = jnp.concatenate([key] * PACK, axis=0) * own
            scores = lax.dot_general(
                query, keys, (((1,), (1,)), ((), ())), preferred_element_type=f32
            )
            probs_ref[chunk * group_size : (chunk + 1) * group_size, :] = jnp.exp2(scores * scale)
        weights = probs_ref[...]
        total = jnp.dot(jnp.minimum(weights, top).astype(bf16), same, preferred_element_type=f32)
        probs = (weights / total).astype(bf16)
        for chunk in range(chunks):
            lo = chunk * LANES
            value = qkv_ref[rows, 2 * channels + lo : 2 * channels + lo + LANES]
            values = jnp.concatenate([value] * PACK, axis=0) * own
            mixed_ref[rows, lo : lo + LANES] = jnp.dot(
                probs[chunk * group_size : (chunk + 1) * group_size],
                values,
                preferred_element_type=f32,
            ).astype(bf16)
        return carry

    lax.fori_loop(0, count // group_size, one_group, 0)
    place = (column == place_ref[...]).astype(f32).astype(bf16)
    result = jnp.dot(mixed_ref[...], out_weight_ref[...], preferred_element_type=f32)
    result = (result + out_bias_ref[...]).astype(bf16)
    o_ref[...] = jnp.dot(place, result, preferred_element_type=f32).astype(bf16)


def attend(tokens, order, group_size, qkv_weight, qkv_bias, out_weight, out_bias):
    count, channels = tokens.shape
    pick = np.asarray(order, np.int32)
    place = np.argsort(pick).astype(np.int32)
    whole = pl.BlockSpec(memory_space=pltpu.VMEM)
    return pl.pallas_call(
        functools.partial(attend_kernel, group_size),
        out_shape=jax.ShapeDtypeStruct((count, channels), jnp.bfloat16),
        in_specs=[whole] * 7,
        out_specs=whole,
        scratch_shapes=[
            pltpu.VMEM((count, 3 * channels), jnp.bfloat16),
            pltpu.VMEM((count, channels), jnp.bfloat16),
            pltpu.VMEM((channels // LANES * group_size, PACK * group_size), jnp.float32),
        ],
        cost_estimate=pl.CostEstimate(
            flops=10 * count * channels * channels, bytes_accessed=8 << 20, transcendentals=1 << 20
        ),
        compiler_params=pltpu.CompilerParams(vmem_limit_bytes=40 << 20),
        name="grid_attention",
    )(
        tokens,
        jnp.asarray(pick)[:, None],
        jnp.asarray(place)[:, None],
        qkv_weight,
        qkv_bias[None],
        out_weight,
        out_bias[None],
    )


def per_device(
    features,
    norm_scale,
    norm_shift,
    expand_weight,
    expand_bias,
    depth_kernel,
    depth_bias,
    project_weight,
    project_bias,
    attn_gain,
    attn_shift,
    qkv_weight,
    qkv_bias,
    out_weight,
    out_bias,
):
    tile_rows, tile_cols, channels = features.shape
    row_count = lax.axis_size("row")
    col_count = lax.axis_size("col")
    row_at = lax.axis_index("row")
    col_at = lax.axis_index("col")
    around = extended(features, (("row", 0), ("col", 1)), 1)
    padded = expand_cells(around, norm_scale, norm_shift, expand_weight, expand_bias)
    height = jnp.arange(tile_rows + 2) + row_at * tile_rows
    width = jnp.arange(tile_cols + 2) + col_at * tile_cols
    inside = ((height >= 1) & (height <= tile_rows * row_count))[:, None] & (
        (width >= 1) & (width <= tile_cols * col_count)
    )[None, :]
    padded = jnp.where(inside[..., None], padded, 0)
    summed = jnp.zeros((tile_rows, tile_cols, padded.shape[-1]), jnp.float32)
    for row_off in range(3):
        for col_off in range(3):
            summed = (
                summed
                + padded[row_off : row_off + tile_rows, col_off : col_off + tile_cols].astype(
                    jnp.float32
                )
                * depth_kernel[row_off, col_off]
            )
    depthwise = jax.nn.gelu(summed + depth_bias).astype(jnp.bfloat16)
    projected = (
        jnp.dot(
            depthwise.reshape(-1, depthwise.shape[-1]),
            project_weight,
            preferred_element_type=jnp.float32,
        )
        + project_bias
    )
    after_conv = (
        features.astype(jnp.float32) + projected.reshape(tile_rows, tile_cols, channels)
    ).astype(jnp.bfloat16)
    attn_in = layer_norm(after_conv, attn_gain, attn_shift)
    fold_row = max(1, GRID // row_count)
    fold_col = max(1, GRID // col_count)
    parity_row = max(1, row_count // GRID)
    parity_col = max(1, col_count // GRID)
    block_row = tile_rows // (fold_row * row_count)
    block_col = tile_cols // (fold_col * col_count)
    tile_view = attn_in.reshape(
        fold_row, row_count, block_row, fold_col, col_count, block_col, channels
    )
    ordered = tile_view.transpose(1, 4, 0, 2, 3, 5, 6).reshape(
        row_count * col_count, fold_row, block_row, fold_col, block_col, channels
    )
    received = lax.all_to_all(ordered, ("row", "col"), split_axis=0, concat_axis=0, tiled=True)
    tokens = received.reshape(-1, channels)
    layout = np.arange(tokens.shape[0]).reshape(
        row_count // parity_row,
        parity_row,
        col_count // parity_col,
        parity_col,
        fold_row,
        block_row,
        fold_col,
        block_col,
    )
    order = layout.transpose(1, 3, 5, 7, 0, 2, 4, 6)
    group_size = math.prod(order.shape[4:])
    answered = attend(
        tokens, order.reshape(-1), group_size, qkv_weight, qkv_bias, out_weight, out_bias
    ).reshape(received.shape)
    returned = lax.all_to_all(answered, ("row", "col"), split_axis=0, concat_axis=0, tiled=True)
    returned_tiles = returned.reshape(
        row_count, col_count, fold_row, block_row, fold_col, block_col, channels
    ).transpose(2, 0, 3, 4, 1, 5, 6)
    attended = returned_tiles.reshape(tile_rows, tile_cols, channels)
    return (after_conv.astype(jnp.float32) + attended.astype(jnp.float32)).astype(jnp.bfloat16)


def solution(mesh):
    return jax.shard_map(
        per_device,
        mesh=mesh,
        in_specs=(P("row", "col", None),) + (P(),) * 14,
        out_specs=P("row", "col", None),
        check_vma=False,
    )
```

```python
import functools
import math

import jax
import jax.numpy as jnp
import numpy as np
from jax import lax
from jax.experimental import pallas as pl
from jax.experimental.pallas import tpu as pltpu
from jax.sharding import PartitionSpec as P

HEADS = 24
HEAD_DIM = 32
GRID = 8
LANES = 128
PACK = LANES // HEAD_DIM


def gelu(v):
    half = 0.5 * v
    inner = v * (0.7978845608028654 + 0.035677408136300125 * (v * v))
    return half + half * jnp.tanh(inner)


def in_hbm(array):
    return pltpu.with_memory_space_constraint(array, pltpu.HBM)


def row_of(ref, cols=slice(None)):
    return ref[cols].reshape(1, -1)


def fetch(source, target, sems, start, count):
    block = target.shape[-1]
    return [
        pltpu.make_async_copy(
            source.at[:, pl.ds((start + i) * block, block)], target.at[i], sems.at[i]
        )
        for i in range(count)
    ]


FOLD = 8


def one_hot(index_ref, count):
    column = lax.broadcasted_iota(jnp.int32, (index_ref.shape[0], count), 1)
    return (column == index_ref[...]).astype(jnp.float32).astype(jnp.bfloat16)


def shuffled(index_ref, values):
    pick = one_hot(index_ref, values.shape[0])
    return jnp.dot(pick, values, preferred_element_type=jnp.float32).astype(jnp.bfloat16)


def whole(array):
    return pl.BlockSpec(array.shape, lambda i: (0,) * array.ndim)


OUTSIDE = pl.BlockSpec(memory_space=pltpu.HBM)


INSIDE = pl.BlockSpec(memory_space=pltpu.VMEM)
BLOCK = 256
TALL = 128


def like(*arrays):
    return [jax.ShapeDtypeStruct(array.shape, array.dtype) for array in arrays]


def expand_all(start, normed_ref, bias_ref, copies, held_ref, o_ref):
    steps, _, block = held_ref.shape
    count = normed_ref.shape[0]
    for i in range(steps):
        copies[i].wait()
        cols = slice(i * block, (i + 1) * block)
        bias = row_of(bias_ref, slice((start + i) * block, (start + i + 1) * block))
        for lo in range(0, count, TALL):
            rows = slice(lo, lo + TALL)
            part = jnp.dot(normed_ref[rows], held_ref[i], preferred_element_type=jnp.float32)
            o_ref[rows, cols] = gelu(part + bias)


def normalize(x, scale_ref, shift_ref):
    return (x.astype(jnp.float32) * row_of(scale_ref) + row_of(shift_ref)).astype(jnp.bfloat16)


def expand_low_kernel(
    x_ref,
    fold_ref,
    columns_ref,
    scale_ref,
    shift_ref,
    bias_ref,
    weight_ref,
    o_ref,
    folded_ref,
    edges_ref,
    held_ref,
    normed_ref,
    sems,
):
    copies = fetch(weight_ref, held_ref, sems, 0, held_ref.shape[0])
    for copy in copies:
        copy.start()
    x = x_ref[...]
    folded = shuffled(fold_ref, x)
    folded_ref[...] = folded
    edges_ref[...] = shuffled(columns_ref, x)
    normed_ref[...] = normalize(folded, scale_ref, shift_ref)
    expand_all(0, normed_ref, bias_ref, copies, held_ref, o_ref)


def expand_high_kernel(
    scale_ref,
    shift_ref,
    bias_ref,
    folded_ref,
    _,
    weight_ref,
    project_ref,
    o_ref,
    held_ref,
    project_held_ref,
    normed_ref,
    sems,
    project_sem,
):
    steps = held_ref.shape[0]
    copies = fetch(weight_ref, held_ref, sems, steps, steps)
    project = pltpu.make_async_copy(project_ref, project_held_ref, project_sem)
    for copy in copies:
        copy.start()
    project.start()
    normed_ref[...] = normalize(folded_ref[...], scale_ref, shift_ref)
    expand_all(steps, normed_ref, bias_ref, copies, held_ref, o_ref)
    project.wait()


def expand_low(fold, columns, tokens, scale, shift, weight, bias):
    count, channels = tokens.shape
    width = weight.shape[1] // 2
    steps = width // BLOCK
    smalls = [tokens, fold, columns, scale, shift, bias]
    return pl.pallas_call(
        expand_low_kernel,
        grid=(1,),
        out_shape=[
            jax.ShapeDtypeStruct((count, width), jnp.float32),
            jax.ShapeDtypeStruct((count, channels), jnp.bfloat16),
            jax.ShapeDtypeStruct((columns.shape[0], channels), jnp.bfloat16),
            jax.ShapeDtypeStruct((steps, channels, BLOCK), jnp.bfloat16),
        ],
        in_specs=[whole(array) for array in smalls] + [OUTSIDE],
        out_specs=[INSIDE] * 4,
        scratch_shapes=[
            pltpu.VMEM((count, channels), jnp.bfloat16),
            pltpu.SemaphoreType.DMA((steps,)),
        ],
        cost_estimate=pl.CostEstimate(
            flops=2 * count * channels * width,
            bytes_accessed=2 * channels * width,
            transcendentals=count * width,
        ),
        compiler_params=pltpu.CompilerParams(vmem_limit_bytes=12 << 20),
        name="expand_low",
    )(*[in_hbm(array) for array in smalls], in_hbm(weight))


def expand_high(folded, after, scale, shift, weight, bias, project_weight):
    count, channels = folded.shape
    width = weight.shape[1] // 2
    steps = width // BLOCK
    smalls = [scale, shift, bias]
    return pl.pallas_call(
        expand_high_kernel,
        grid=(1,),
        out_shape=[
            jax.ShapeDtypeStruct((count, width), jnp.float32),
            jax.ShapeDtypeStruct((steps, channels, BLOCK), jnp.bfloat16),
            *like(project_weight),
        ],
        in_specs=[whole(array) for array in smalls]
        + [INSIDE, pl.BlockSpec(memory_space=pl.ANY), OUTSIDE, OUTSIDE],
        out_specs=[INSIDE] * 3,
        scratch_shapes=[
            pltpu.VMEM((count, channels), jnp.bfloat16),
            pltpu.SemaphoreType.DMA((steps,)),
            pltpu.SemaphoreType.DMA,
        ],
        cost_estimate=pl.CostEstimate(
            flops=2 * count * channels * width,
            bytes_accessed=6 * channels * width,
            transcendentals=count * width,
        ),
        compiler_params=pltpu.CompilerParams(vmem_limit_bytes=12 << 20),
        name="expand_high",
    )(*[in_hbm(array) for array in smalls], folded, after, in_hbm(weight), in_hbm(project_weight))


def edges_kernel(tall, first_row_ref, second_row_ref, edges_ref, first_ref, second_ref):
    f32 = jnp.float32
    row_even = lax.rem(lax.axis_index("row"), 2) == 0
    col_even = lax.rem(lax.axis_index("col"), 2) == 0
    strip = first_ref.shape[0]
    last = first_row_ref.shape[0]
    spot = lax.broadcasted_iota(jnp.int32, (strip, 1), 0)

    def column(side, at):
        first = first_row_ref[at : at + 1].astype(f32)
        second = second_row_ref[at : at + 1].astype(f32)
        top = jnp.where(row_even, second, first)
        bottom = jnp.where(row_even, first, second)
        middle = edges_ref[side * strip : (side + 1) * strip].astype(f32)
        return jnp.where(spot == 0, top, jnp.where(spot == tall - 1, bottom, middle))

    left, right = column(0, 0), column(1, last - 1)
    first_ref[...] = jnp.where(col_even, right, left).astype(jnp.bfloat16)
    second_ref[...] = jnp.where(col_even, left, right).astype(jnp.bfloat16)


def edges_to_send(tall, first_row, second_row, edges):
    shape = jax.ShapeDtypeStruct((edges.shape[0] // 2, edges.shape[1]), edges.dtype)
    return pl.pallas_call(
        functools.partial(edges_kernel, tall),
        out_shape=[shape, shape],
        in_specs=[INSIDE] * 3,
        out_specs=[INSIDE] * 2,
        compiler_params=pltpu.CompilerParams(vmem_limit_bytes=2 << 20),
        name="edges",
    )(first_row, second_row, edges)


def conv_kernel(
    shape,
    halo_order_ref,
    natural_ref,
    order_ref,
    scale_ref,
    shift_ref,
    expand_bias_ref,
    depth_kernel_ref,
    depth_bias_ref,
    project_bias_ref,
    gain_ref,
    offset_ref,
    low_ref,
    high_ref,
    first_row_ref,
    second_row_ref,
    first_col_ref,
    second_col_ref,
    low_weight_ref,
    high_weight_ref,
    project_weight_ref,
    features_ref,
    qkv_weight_ref,
    out_weight_ref,
    after_ref,
    attn_ref,
    qkv_held_ref,
    out_held_ref,
    normed_ref,
    halo_hidden_ref,
    left_ref,
    right_ref,
    depth_ref,
    sems,
):
    f32, bf16 = jnp.float32, jnp.bfloat16
    rows, cols = shape
    planes = cols // FOLD
    tall = rows + 2
    strip = first_col_ref.shape[0]
    prefetch = [
        pltpu.make_async_copy(qkv_weight_ref, qkv_held_ref, sems.at[0]),
        pltpu.make_async_copy(out_weight_ref, out_held_ref, sems.at[1]),
    ]
    for copy in prefetch:
        copy.start()

    row_at, col_at = lax.axis_index("row"), lax.axis_index("col")
    row_even, col_even = lax.rem(row_at, 2) == 0, lax.rem(col_at, 2) == 0
    has_top = (row_at > 0).astype(f32)
    has_bottom = (row_at < lax.axis_size("row") - 1).astype(f32)
    has_left = (col_at > 0).astype(f32)
    has_right = (col_at < lax.axis_size("col") - 1).astype(f32)
    top_at = jnp.where(row_even, cols, 0)
    bottom_at = jnp.where(row_even, 0, cols)
    left_at = 2 * cols + jnp.where(col_even, strip, 0)
    right_at = 2 * cols + jnp.where(col_even, 0, strip)
    spot = lax.broadcasted_iota(jnp.int32, (2 * cols + 2 * strip, 1), 0)
    first_there = jnp.where(row_even, has_bottom, has_top)
    second_there = jnp.where(row_even, has_top, has_bottom)
    near_there = jnp.where(col_even, has_right, has_left)
    far_there = jnp.where(col_even, has_left, has_right)
    place = lax.rem(spot, strip)
    ends = jnp.where(place == 0, has_top, jnp.where(place == tall - 1, has_bottom, 1.0))
    keep = jnp.where(
        spot < cols,
        first_there,
        jnp.where(
            spot < 2 * cols,
            second_there,
            ends * jnp.where(spot < 2 * cols + strip, near_there, far_there),
        ),
    )

    halo = jnp.concatenate(
        [first_row_ref[...], second_row_ref[...], first_col_ref[...], second_col_ref[...]], axis=0
    )
    normed_ref[...] = shuffled(halo_order_ref, normalize(halo, scale_ref, shift_ref))

    def convolve(step, hidden_ref, weight_ref, offset):
        base = pl.multiple_of((step + offset) * BLOCK, BLOCK)
        part = jnp.dot(normed_ref[...], weight_ref[step], preferred_element_type=f32)
        bias = expand_bias_ref[pl.ds(base, BLOCK)].reshape(1, BLOCK)
        halo_hidden_ref[...] = gelu(part + bias) * keep
        for lane in range(BLOCK // LANES):
            lanes = slice(lane * LANES, (lane + 1) * LANES)
            inner = pl.ds(pl.multiple_of(step * BLOCK + lane * LANES, LANES), LANES)
            outer = pl.ds(pl.multiple_of(base + lane * LANES, LANES), LANES)
            left = halo_hidden_ref[pl.ds(pl.multiple_of(left_at, 8), strip), lanes]
            right = halo_hidden_ref[pl.ds(pl.multiple_of(right_at, 8), strip), lanes]

            def cell(r, j):
                if r == 0 or r == tall - 1:
                    at = (top_at if r == 0 else bottom_at) + j * FOLD
                    return halo_hidden_ref[pl.ds(pl.multiple_of(at, 8), FOLD), lanes]
                at = ((r - 1) * planes + j) * FOLD
                return hidden_ref[at : at + FOLD, inner]

            for r in range(tall):
                left_ref[lane, r, 8 : 8 + FOLD, :] = cell(r, planes - 1)
                left_ref[lane, r, 7:8, :] = left[r : r + 1]
                right_ref[lane, r, 0:FOLD, :] = cell(r, 0)
                right_ref[lane, r, FOLD : FOLD + 1, :] = right[r : r + 1]

            def shifted(r, j):
                if j < 0:
                    return left_ref[lane, r, 7 : 7 + FOLD, :]
                if j == planes:
                    return right_ref[lane, r, 1 : 1 + FOLD, :]
                return cell(r, j)

            taps = [
                [
                    jnp.broadcast_to(depth_kernel_ref[a, b : b + 1, outer], (FOLD, LANES))
                    for b in range(3)
                ]
                for a in range(3)
            ]
            bias = jnp.broadcast_to(depth_bias_ref[outer].reshape(1, LANES), (FOLD, LANES))
            pair = 2
            for start in range(0, planes, pair):
                sums = [[None] * rows for _ in range(pair)]
                for r in range(tall):
                    near = [shifted(r, start - 1 + b) for b in range(pair + 2)]
                    for k in range(pair):
                        for a in range(3):
                            h = r - a
                            if 0 <= h < rows:
                                line = near[k] * taps[a][0] + near[k + 1] * taps[a][1]
                                line = line + near[k + 2] * taps[a][2]
                                old = sums[k][h]
                                sums[k][h] = line + (bias if old is None else old)
                    h = r - 2
                    if h >= 0:
                        lo = (h * planes + start) * FOLD
                        depth_ref[lo : lo + pair * FOLD, outer] = jnp.concatenate(
                            [gelu(sums[k][h]) for k in range(pair)], axis=0
                        ).astype(bf16)

    half = low_weight_ref.shape[0]

    def low_step(step, carry):
        convolve(step, low_ref, low_weight_ref, 0)
        return carry

    def high_step(step, carry):
        convolve(step, high_ref, high_weight_ref, half)
        return carry

    lax.fori_loop(0, half, low_step, 0)
    lax.fori_loop(0, half, high_step, 0)

    group = 256
    normals, afters = [], []
    for lo in range(0, rows * cols, group):
        part = slice(lo, lo + group)
        total = jnp.dot(depth_ref[part], project_weight_ref[...], preferred_element_type=f32)
        after = features_ref[part].astype(f32) + total + row_of(project_bias_ref)
        after = after.astype(bf16)
        wide = after.astype(f32)
        center = wide - jnp.mean(wide, axis=-1, keepdims=True)
        spread = jnp.mean(center * center, axis=-1, keepdims=True)
        normal = center * lax.rsqrt(spread + 1e-06) * row_of(gain_ref) + row_of(offset_ref)
        afters.append(after)
        normals.append(normal.astype(bf16))
    after_ref[...] = shuffled(natural_ref, jnp.concatenate(afters, axis=0))
    attn_ref[...] = shuffled(order_ref, jnp.concatenate(normals, axis=0))
    for copy in prefetch:
        copy.wait()


def convolve(shape, smalls, larges, qkv_weight, out_weight):
    rows, cols = shape
    features = larges[-1]
    count, channels = features.shape
    width = larges[0].shape[1] * 2
    around = smalls[0].shape[0]
    return pl.pallas_call(
        functools.partial(conv_kernel, shape),
        grid=(1,),
        out_shape=like(features, features, qkv_weight, out_weight),
        in_specs=[whole(array) for array in smalls] + [INSIDE] * len(larges) + [OUTSIDE] * 2,
        out_specs=[INSIDE] * 4,
        scratch_shapes=[
            pltpu.VMEM((around, channels), jnp.bfloat16),
            pltpu.VMEM((around, BLOCK), jnp.float32),
            pltpu.VMEM((BLOCK // LANES, rows + 2, FOLD + 8, LANES), jnp.float32),
            pltpu.VMEM((BLOCK // LANES, rows + 2, FOLD + 8, LANES), jnp.float32),
            pltpu.VMEM((count, width), jnp.bfloat16),
            pltpu.SemaphoreType.DMA((2,)),
        ],
        cost_estimate=pl.CostEstimate(
            flops=4 * count * channels * width,
            bytes_accessed=4 * channels * width,
            transcendentals=count * width,
        ),
        compiler_params=pltpu.CompilerParams(vmem_limit_bytes=24 << 20),
        name="depthwise_project",
    )(*[in_hbm(array) for array in smalls], *larges, in_hbm(qkv_weight), in_hbm(out_weight))


def swap(cells, axis, count, odd_pairs):
    pairs = [(i, i + 1) for i in range(1 if odd_pairs else 0, count - 1, 2)]
    return lax.ppermute(cells, axis, pairs + [(j, i) for i, j in pairs])


def attend_kernel(
    group_size,
    x_ref,
    pick_ref,
    place_ref,
    qkv_weight_ref,
    qkv_bias_ref,
    out_weight_ref,
    out_bias_ref,
    o_ref,
    qkv_ref,
    mixed_ref,
    probs_ref,
):
    count, channels = x_ref.shape
    f32, bf16 = jnp.float32, jnp.bfloat16
    x = shuffled(pick_ref, x_ref[...])
    step = 256
    for lo in range(0, 3 * channels, step):
        cols = slice(lo, lo + step)
        part = jnp.dot(x, qkv_weight_ref[:, cols], preferred_element_type=f32)
        qkv_ref[:, cols] = (part + row_of(qkv_bias_ref, cols)).astype(bf16)

    wide = PACK * group_size
    lane = lax.broadcasted_iota(jnp.int32, (wide, LANES), 1) // HEAD_DIM
    row = lax.broadcasted_iota(jnp.int32, (wide, LANES), 0) // group_size
    own = (lane == row).astype(f32).astype(bf16)
    block_row = lax.broadcasted_iota(jnp.int32, (wide, wide), 0) // group_size
    block_col = lax.broadcasted_iota(jnp.int32, (wide, wide), 1) // group_size
    same = (block_row == block_col).astype(f32).astype(bf16)
    scale = math.log2(math.e) / math.sqrt(HEAD_DIM)
    top = float(jnp.finfo(bf16).max)
    chunks = channels // LANES

    def one_group(group, carry):
        rows = pl.ds(pl.multiple_of(group * group_size, group_size), group_size)
        for chunk in range(chunks):
            lo = chunk * LANES
            query = qkv_ref[rows, lo : lo + LANES]
            key = qkv_ref[rows, channels + lo : channels + lo + LANES]
            keys = jnp.concatenate([key] * PACK, axis=0) * own
            scores = lax.dot_general(
                query, keys, (((1,), (1,)), ((), ())), preferred_element_type=f32
            )
            probs_ref[chunk * group_size : (chunk + 1) * group_size, :] = jnp.exp2(scores * scale)
        weights = probs_ref[...]
        total = jnp.dot(jnp.minimum(weights, top).astype(bf16), same, preferred_element_type=f32)
        probs = (weights / total).astype(bf16)
        for chunk in range(chunks):
            lo = chunk * LANES
            value = qkv_ref[rows, 2 * channels + lo : 2 * channels + lo + LANES]
            values = jnp.concatenate([value] * PACK, axis=0) * own
            mixed_ref[rows, lo : lo + LANES] = jnp.dot(
                probs[chunk * group_size : (chunk + 1) * group_size],
                values,
                preferred_element_type=f32,
            ).astype(bf16)
        return carry

    lax.fori_loop(0, count // group_size, one_group, 0)
    result = jnp.dot(mixed_ref[...], out_weight_ref[...], preferred_element_type=f32)
    o_ref[...] = shuffled(place_ref, (result + row_of(out_bias_ref)).astype(bf16))


def attend(tokens, order, group_size, qkv_weight, qkv_bias, out_weight, out_bias):
    count, channels = tokens.shape
    pick = np.asarray(order, np.int32)
    place = np.argsort(pick).astype(np.int32)
    inside = pl.BlockSpec(memory_space=pltpu.VMEM)
    smalls = [jnp.asarray(pick)[:, None], jnp.asarray(place)[:, None], qkv_bias, out_bias]
    pick, place, qkv_bias, out_bias = [in_hbm(array) for array in smalls]
    arrays = [tokens, pick, place, qkv_weight, qkv_bias, out_weight, out_bias]
    specs = [whole(array) for array in arrays]
    specs[0] = specs[3] = specs[5] = inside
    return pl.pallas_call(
        functools.partial(attend_kernel, group_size),
        grid=(1,),
        out_shape=jax.ShapeDtypeStruct((count, channels), jnp.bfloat16),
        in_specs=specs,
        out_specs=inside,
        scratch_shapes=[
            pltpu.VMEM((count, 3 * channels), jnp.bfloat16),
            pltpu.VMEM((count, channels), jnp.bfloat16),
            pltpu.VMEM((channels // LANES * group_size, PACK * group_size), jnp.float32),
        ],
        cost_estimate=pl.CostEstimate(
            flops=10 * count * channels * channels, bytes_accessed=8 << 20, transcendentals=1 << 20
        ),
        compiler_params=pltpu.CompilerParams(vmem_limit_bytes=16 << 20),
        name="grid_attention",
    )(*arrays)


def per_device(
    features,
    norm_scale,
    norm_shift,
    expand_weight,
    expand_bias,
    depth_kernel,
    depth_bias,
    project_weight,
    project_bias,
    attn_gain,
    attn_shift,
    qkv_weight,
    qkv_bias,
    out_weight,
    out_bias,
):
    tile_rows, tile_cols, channels = features.shape
    row_count = lax.axis_size("row")
    col_count = lax.axis_size("col")
    row_at = lax.axis_index("row")
    flat = features.reshape(-1, channels)
    tall = tile_rows + 2
    strip = -(-tall // 16) * 16
    planes = tile_cols // FOLD
    one_row = np.arange(tile_cols).reshape(FOLD, planes).T.reshape(-1)
    fold = (np.arange(tile_rows)[:, None] * tile_cols + one_row[None]).reshape(-1)
    unfold = np.argsort(fold)
    columns = np.full((2, strip), -1)
    columns[0, 1 : tall - 1] = np.arange(tile_rows) * tile_cols
    columns[1, 1 : tall - 1] = np.arange(tile_rows) * tile_cols + tile_cols - 1

    def index_array(values):
        return jnp.asarray(np.asarray(values, np.int32).reshape(-1))[:, None]

    row_even = row_at % 2 == 0
    near = lax.dynamic_slice_in_dim(features, jnp.where(row_even, tile_rows - 1, 0), 1, 0)[0]
    far = lax.dynamic_slice_in_dim(features, jnp.where(row_even, 0, tile_rows - 1), 1, 0)[0]
    first_row = swap(near, "row", row_count, False)
    second_row = swap(far, "row", row_count, True)
    low, folded, edges, low_weight = expand_low(
        index_array(fold),
        index_array(columns),
        flat,
        norm_scale,
        norm_shift,
        expand_weight,
        expand_bias,
    )
    first_col, second_col = edges_to_send(tall, first_row, second_row, edges)
    high, high_weight, project_held = expand_high(
        folded, first_col, norm_scale, norm_shift, expand_weight, expand_bias, project_weight
    )
    first_col = swap(first_col, "col", col_count, False)
    second_col = swap(second_col, "col", col_count, True)
    fold_row = max(1, GRID // row_count)
    fold_col = max(1, GRID // col_count)
    parity_row = max(1, row_count // GRID)
    parity_col = max(1, col_count // GRID)
    block_row = tile_rows // (fold_row * row_count)
    block_col = tile_cols // (fold_col * col_count)
    source = np.arange(tile_rows * tile_cols).reshape(
        fold_row, row_count, block_row, fold_col, col_count, block_col
    )
    source = source.transpose(1, 4, 0, 2, 3, 5).reshape(-1)
    around = np.concatenate(
        [one_row, tile_cols + one_row, 2 * tile_cols + np.arange(2 * strip)]
    )
    after_conv, ordered, qkv_weight, out_weight = convolve(
        (tile_rows, tile_cols),
        [
            index_array(around),
            index_array(unfold),
            index_array(unfold[source]),
            norm_scale,
            norm_shift,
            expand_bias,
            depth_kernel,
            depth_bias,
            project_bias,
            attn_gain,
            attn_shift,
        ],
        [
            low,
            high,
            first_row,
            second_row,
            first_col,
            second_col,
            low_weight,
            high_weight,
            project_held,
            folded,
        ],
        qkv_weight,
        out_weight,
    )
    after_conv = after_conv.reshape(features.shape)
    ordered = ordered.reshape(
        row_count * col_count, fold_row, block_row, fold_col, block_col, channels
    )
    received = lax.all_to_all(ordered, ("row", "col"), split_axis=0, concat_axis=0, tiled=True)
    tokens = received.reshape(-1, channels)
    layout = np.arange(tokens.shape[0]).reshape(
        row_count // parity_row,
        parity_row,
        col_count // parity_col,
        parity_col,
        fold_row,
        block_row,
        fold_col,
        block_col,
    )
    order = layout.transpose(1, 3, 5, 7, 0, 2, 4, 6)
    group_size = math.prod(order.shape[4:])
    answered = attend(
        tokens, order.reshape(-1), group_size, qkv_weight, qkv_bias, out_weight, out_bias
    ).reshape(received.shape)
    returned = lax.all_to_all(answered, ("row", "col"), split_axis=0, concat_axis=0, tiled=True)
    returned_tiles = returned.reshape(
        row_count, col_count, fold_row, block_row, fold_col, block_col, channels
    ).transpose(2, 0, 3, 4, 1, 5, 6)
    attended = returned_tiles.reshape(tile_rows, tile_cols, channels)
    return (after_conv.astype(jnp.float32) + attended.astype(jnp.float32)).astype(jnp.bfloat16)


def solution(mesh):
    return jax.shard_map(
        per_device,
        mesh=mesh,
        in_specs=(P("row", "col", None),) + (P(),) * 14,
        out_specs=P("row", "col", None),
        check_vma=False,
    )
```

```python
import functools
import math

import jax
import jax.numpy as jnp
import numpy as np
from jax import lax
from jax.experimental import pallas as pl
from jax.experimental.pallas import tpu as pltpu
from jax.sharding import PartitionSpec as P

HEADS = 24
HEAD_DIM = 32
GRID = 8
LANES = 128
PACK = LANES // HEAD_DIM
TOGETHER = 2


def gelu(v):
    half = 0.5 * v
    inner = v * (0.7978845608028654 + 0.035677408136300125 * (v * v))
    return half + half * jnp.tanh(inner)


def in_hbm(array):
    return pltpu.with_memory_space_constraint(array, pltpu.HBM)


def row_of(ref, cols=slice(None)):
    return ref[cols].reshape(1, -1)


def fetch(source, target, sems, start, count):
    block = target.shape[-1]
    return [
        pltpu.make_async_copy(
            source.at[:, pl.ds((start + i) * block, block)], target.at[i], sems.at[i]
        )
        for i in range(count)
    ]


FOLD = 8


def shuffled(target_ref, values, count=None):
    shape = (count or values.shape[0], values.shape[0])
    row = lax.broadcasted_iota(jnp.int32, shape, 0)
    pick = (row == target_ref[...]).astype(jnp.float32).astype(jnp.bfloat16)
    return jnp.dot(pick, values, preferred_element_type=jnp.float32).astype(jnp.bfloat16)


def whole(array):
    return pl.BlockSpec(array.shape, lambda i: (0,) * array.ndim)


OUTSIDE = pl.BlockSpec(memory_space=pltpu.HBM)


INSIDE = pl.BlockSpec(memory_space=pltpu.VMEM)
BLOCK = 256
TWO = 2
WIDE = TWO * BLOCK
TALL = 128


def like(*arrays):
    return [jax.ShapeDtypeStruct(array.shape, array.dtype) for array in arrays]


def expand_all(start, normed_ref, bias_ref, copies, held_ref, o_ref):
    steps, _, block = held_ref.shape
    count = normed_ref.shape[0]
    for i in range(steps):
        copies[i].wait()
        cols = slice(i * block, (i + 1) * block)
        bias = row_of(bias_ref, slice((start + i) * block, (start + i + 1) * block))
        for lo in range(0, count, TALL):
            rows = slice(lo, lo + TALL)
            part = jnp.dot(normed_ref[rows], held_ref[i], preferred_element_type=jnp.float32)
            o_ref[rows, cols] = gelu(part + bias)


def normalize(x, scale_ref, shift_ref):
    return (x.astype(jnp.float32) * row_of(scale_ref) + row_of(shift_ref)).astype(jnp.bfloat16)


def expand_low_kernel(smalls, *refs):
    x_ref, fold_ref, columns_ref, weight_ref, *refs = refs
    sources, refs = refs[:smalls], refs[smalls:]
    o_ref, folded_ref, edges_ref, held_ref, *refs = refs
    targets, refs = refs[:smalls], refs[smalls:]
    x_held_ref, fold_held_ref, columns_held_ref, normed_ref, sems, first_sems, small_sems = refs
    firsts = [
        pltpu.make_async_copy(source, target, first_sems.at[i])
        for i, (source, target) in enumerate(
            [
                (x_ref, x_held_ref),
                (fold_ref, fold_held_ref),
                (columns_ref, columns_held_ref),
            ]
        )
    ]
    hand_on = [
        pltpu.make_async_copy(source, target, small_sems.at[i])
        for i, (source, target) in enumerate(zip(sources, targets, strict=True))
    ]
    copies = fetch(weight_ref, held_ref, sems, 0, held_ref.shape[0])
    needed = 3
    for copy in firsts + hand_on[:needed] + copies + hand_on[needed:]:
        copy.start()
    for copy in firsts + hand_on[:needed]:
        copy.wait()
    scale_ref, shift_ref, bias_ref = targets[:needed]
    x = x_held_ref[...]
    folded = shuffled(fold_held_ref, x)
    folded_ref[...] = folded
    edges_ref[...] = shuffled(columns_held_ref, x, edges_ref.shape[0])
    normed_ref[...] = normalize(folded, scale_ref, shift_ref)
    expand_all(0, normed_ref, bias_ref, copies, held_ref, o_ref)
    for copy in hand_on[needed:]:
        copy.wait()


def expand_high_kernel(
    scale_ref, shift_ref, bias_ref, folded_ref, _, weight_ref, o_ref, held_ref, normed_ref, sems
):
    steps = held_ref.shape[0]
    copies = fetch(weight_ref, held_ref, sems, steps, steps)
    for copy in copies:
        copy.start()
    normed_ref[...] = normalize(folded_ref[...], scale_ref, shift_ref)
    expand_all(steps, normed_ref, bias_ref, copies, held_ref, o_ref)


def expand_low(fold, columns, edge_count, tokens, weight, smalls):
    count, channels = tokens.shape
    width = weight.shape[1] // 2
    steps = width // BLOCK
    arrays = [tokens, fold, columns, weight, *smalls]
    shapes = [
        jax.ShapeDtypeStruct((count, width), jnp.float32),
        jax.ShapeDtypeStruct((count, channels), jnp.bfloat16),
        jax.ShapeDtypeStruct((edge_count, channels), jnp.bfloat16),
        jax.ShapeDtypeStruct((steps, channels, BLOCK), jnp.bfloat16),
        *like(*smalls),
    ]
    return pl.pallas_call(
        functools.partial(expand_low_kernel, len(smalls)),
        out_shape=shapes,
        in_specs=[OUTSIDE] * len(arrays),
        out_specs=[INSIDE] * len(shapes),
        scratch_shapes=[
            pltpu.VMEM(tokens.shape, tokens.dtype),
            pltpu.VMEM(fold.shape, fold.dtype),
            pltpu.VMEM(columns.shape, columns.dtype),
            pltpu.VMEM((count, channels), jnp.bfloat16),
            pltpu.SemaphoreType.DMA((steps,)),
            pltpu.SemaphoreType.DMA((3,)),
            pltpu.SemaphoreType.DMA((len(smalls),)),
        ],
        cost_estimate=pl.CostEstimate(
            flops=2 * count * channels * width,
            bytes_accessed=2 * channels * width,
            transcendentals=count * width,
        ),
        compiler_params=pltpu.CompilerParams(vmem_limit_bytes=12 << 20),
        name="expand_low",
    )(*[in_hbm(array) for array in arrays])


def expand_high(folded, after, scale, shift, weight, bias):
    count, channels = folded.shape
    width = weight.shape[1] // 2
    steps = width // BLOCK
    return pl.pallas_call(
        expand_high_kernel,
        out_shape=[
            jax.ShapeDtypeStruct((count, width), jnp.float32),
            jax.ShapeDtypeStruct((steps, channels, BLOCK), jnp.bfloat16),
        ],
        in_specs=[INSIDE] * 4 + [pl.BlockSpec(memory_space=pl.ANY), OUTSIDE],
        out_specs=[INSIDE] * 2,
        scratch_shapes=[
            pltpu.VMEM((count, channels), jnp.bfloat16),
            pltpu.SemaphoreType.DMA((steps,)),
        ],
        cost_estimate=pl.CostEstimate(
            flops=2 * count * channels * width,
            bytes_accessed=6 * channels * width,
            transcendentals=count * width,
        ),
        compiler_params=pltpu.CompilerParams(vmem_limit_bytes=12 << 20),
        name="expand_high",
    )(scale, shift, bias, folded, after, in_hbm(weight))


def edges_kernel(tall, first_row_ref, second_row_ref, edges_ref, first_ref, second_ref):
    f32 = jnp.float32
    row_even = lax.rem(lax.axis_index("row"), 2) == 0
    col_even = lax.rem(lax.axis_index("col"), 2) == 0
    strip = first_ref.shape[0]
    last = first_row_ref.shape[0]
    spot = lax.broadcasted_iota(jnp.int32, (strip, 1), 0)

    def column(side, at):
        first = first_row_ref[at : at + 1].astype(f32)
        second = second_row_ref[at : at + 1].astype(f32)
        top = jnp.where(row_even, second, first)
        bottom = jnp.where(row_even, first, second)
        middle = edges_ref[side * strip : (side + 1) * strip].astype(f32)
        return jnp.where(spot == 0, top, jnp.where(spot == tall - 1, bottom, middle))

    left, right = column(0, 0), column(1, last - 1)
    first_ref[...] = jnp.where(col_even, right, left).astype(jnp.bfloat16)
    second_ref[...] = jnp.where(col_even, left, right).astype(jnp.bfloat16)


def edges_to_send(tall, first_row, second_row, edges):
    shape = jax.ShapeDtypeStruct((edges.shape[0] // 2, edges.shape[1]), edges.dtype)
    return pl.pallas_call(
        functools.partial(edges_kernel, tall),
        out_shape=[shape, shape],
        in_specs=[INSIDE] * 3,
        out_specs=[INSIDE] * 2,
        compiler_params=pltpu.CompilerParams(vmem_limit_bytes=2 << 20),
        name="edges",
    )(first_row, second_row, edges)


def conv_kernel(
    shape,
    halo_order_ref,
    natural_ref,
    order_ref,
    scale_ref,
    shift_ref,
    expand_bias_ref,
    depth_kernel_ref,
    depth_bias_ref,
    project_bias_ref,
    gain_ref,
    offset_ref,
    low_ref,
    high_ref,
    first_row_ref,
    second_row_ref,
    first_col_ref,
    second_col_ref,
    low_weight_ref,
    high_weight_ref,
    features_ref,
    project_weight_ref,
    qkv_weight_ref,
    out_weight_ref,
    after_ref,
    attn_ref,
    qkv_held_ref,
    out_held_ref,
    normed_ref,
    halo_hidden_ref,
    left_ref,
    right_ref,
    depth_ref,
    total_ref,
    project_held_ref,
    sems,
    project_sems,
):
    f32, bf16 = jnp.float32, jnp.bfloat16
    rows, cols = shape
    planes = cols // FOLD
    tall = rows + 2
    strip = first_col_ref.shape[0]
    prefetch = [
        pltpu.make_async_copy(qkv_weight_ref, qkv_held_ref, sems.at[0]),
        pltpu.make_async_copy(out_weight_ref, out_held_ref, sems.at[1]),
    ]
    half = low_weight_ref.shape[0] // TWO

    def project_copy(step):
        rows_at = pl.ds(pl.multiple_of(step * WIDE, WIDE), WIDE)
        return pltpu.make_async_copy(
            project_weight_ref.at[rows_at], project_held_ref.at[step], project_sems.at[step]
        )

    for step in range(2 * half):
        project_copy(step).start()
    for copy in prefetch:
        copy.start()

    row_at, col_at = lax.axis_index("row"), lax.axis_index("col")
    row_even, col_even = lax.rem(row_at, 2) == 0, lax.rem(col_at, 2) == 0
    has_top = (row_at > 0).astype(f32)
    has_bottom = (row_at < lax.axis_size("row") - 1).astype(f32)
    has_left = (col_at > 0).astype(f32)
    has_right = (col_at < lax.axis_size("col") - 1).astype(f32)
    top_at = jnp.where(row_even, cols, 0)
    bottom_at = jnp.where(row_even, 0, cols)
    left_at = 2 * cols + jnp.where(col_even, strip, 0)
    right_at = 2 * cols + jnp.where(col_even, 0, strip)
    spot = lax.broadcasted_iota(jnp.int32, (2 * cols + 2 * strip, 1), 0)
    first_there = jnp.where(row_even, has_bottom, has_top)
    second_there = jnp.where(row_even, has_top, has_bottom)
    near_there = jnp.where(col_even, has_right, has_left)
    far_there = jnp.where(col_even, has_left, has_right)
    place = lax.rem(spot, strip)
    ends = jnp.where(place == 0, has_top, jnp.where(place == tall - 1, has_bottom, 1.0))
    keep = jnp.where(
        spot < cols,
        first_there,
        jnp.where(
            spot < 2 * cols,
            second_there,
            ends * jnp.where(spot < 2 * cols + strip, near_there, far_there),
        ),
    )

    halo = jnp.concatenate(
        [first_row_ref[...], second_row_ref[...], first_col_ref[...], second_col_ref[...]], axis=0
    )
    normed_ref[...] = shuffled(halo_order_ref, normalize(halo, scale_ref, shift_ref))

    depth_ref[1] = jnp.zeros_like(depth_ref[1])
    total_ref[...] = features_ref[...].astype(f32) + row_of(project_bias_ref)

    def add_chunk(at, slot):
        total_ref[...] += jnp.dot(
            depth_ref[slot], project_held_ref[at], preferred_element_type=f32
        )

    def convolve(step, hidden_ref, weight_ref, offset):
        slot = lax.rem(step + offset, 2)
        project_copy(step + offset).wait()
        add_chunk(jnp.maximum(step + offset - 1, 0), 1 - slot)
        for sub in range(TWO):
            convolve_block(step * TWO + sub, hidden_ref, weight_ref, offset * TWO, slot, sub)

    def convolve_block(step, hidden_ref, weight_ref, offset, slot, sub):
        base = pl.multiple_of((step + offset) * BLOCK, BLOCK)
        part = jnp.dot(normed_ref[...], weight_ref[step], preferred_element_type=f32)
        bias = expand_bias_ref[pl.ds(base, BLOCK)].reshape(1, BLOCK)
        halo_hidden_ref[sub] = gelu(part + bias) * keep
        for lane in range(BLOCK // LANES):
            lanes = slice(lane * LANES, (lane + 1) * LANES)
            wide_lanes = slice(sub * BLOCK + lane * LANES, sub * BLOCK + (lane + 1) * LANES)
            inner = pl.ds(pl.multiple_of(step * BLOCK + lane * LANES, LANES), LANES)
            outer = pl.ds(pl.multiple_of(base + lane * LANES, LANES), LANES)
            left = halo_hidden_ref[sub, pl.ds(pl.multiple_of(left_at, 8), strip), lanes]
            right = halo_hidden_ref[sub, pl.ds(pl.multiple_of(right_at, 8), strip), lanes]

            def cell(r, j):
                if r == 0 or r == tall - 1:
                    at = (top_at if r == 0 else bottom_at) + j * FOLD
                    return halo_hidden_ref[sub, pl.ds(pl.multiple_of(at, 8), FOLD), lanes]
                at = ((r - 1) * planes + j) * FOLD
                return hidden_ref[at : at + FOLD, inner]

            for r in range(tall):
                left_ref[BLOCK // LANES * sub + lane, r, 8 : 8 + FOLD, :] = cell(r, planes - 1)
                left_ref[BLOCK // LANES * sub + lane, r, 7:8, :] = left[r : r + 1]
                right_ref[BLOCK // LANES * sub + lane, r, 0:FOLD, :] = cell(r, 0)
                right_ref[BLOCK // LANES * sub + lane, r, FOLD : FOLD + 1, :] = right[r : r + 1]

            def shifted(r, j):
                if j < 0:
                    return left_ref[BLOCK // LANES * sub + lane, r, 7 : 7 + FOLD, :]
                if j == planes:
                    return right_ref[BLOCK // LANES * sub + lane, r, 1 : 1 + FOLD, :]
                return cell(r, j)

            taps = [
                [
                    jnp.broadcast_to(depth_kernel_ref[a, b : b + 1, outer], (FOLD, LANES))
                    for b in range(3)
                ]
                for a in range(3)
            ]
            bias = jnp.broadcast_to(depth_bias_ref[outer].reshape(1, LANES), (FOLD, LANES))
            pair = 2
            for start in range(0, planes, pair):
                sums = [[None] * rows for _ in range(pair)]
                for r in range(tall):
                    near = [shifted(r, start - 1 + b) for b in range(pair + 2)]
                    for k in range(pair):
                        for a in range(3):
                            h = r - a
                            if 0 <= h < rows:
                                line = near[k] * taps[a][0] + near[k + 1] * taps[a][1]
                                line = line + near[k + 2] * taps[a][2]
                                old = sums[k][h]
                                sums[k][h] = line + (bias if old is None else old)
                    h = r - 2
                    if h >= 0:
                        lo = (h * planes + start) * FOLD
                        depth_ref[slot, lo : lo + pair * FOLD, wide_lanes] = jnp.concatenate(
                            [gelu(sums[k][h]) for k in range(pair)], axis=0
                        ).astype(bf16)

    def low_step(step, carry):
        convolve(step, low_ref, low_weight_ref, 0)
        return carry

    def high_step(step, carry):
        convolve(step, high_ref, high_weight_ref, half)
        return carry

    lax.fori_loop(0, half, low_step, 0)
    lax.fori_loop(0, half, high_step, 0)

    group = 256
    normals, afters = [], []
    for lo in range(0, rows * cols, group):
        part = slice(lo, lo + group)
        total = total_ref[part] + jnp.dot(
            depth_ref[(2 * half - 1) % 2, part], project_held_ref[2 * half - 1], preferred_element_type=f32
        )
        after = total.astype(bf16)
        wide = after.astype(f32)
        center = wide - jnp.mean(wide, axis=-1, keepdims=True)
        spread = jnp.mean(center * center, axis=-1, keepdims=True)
        normal = center * lax.rsqrt(spread + 1e-06) * row_of(gain_ref) + row_of(offset_ref)
        afters.append(after)
        normals.append(normal.astype(bf16))
    after_ref[...] = shuffled(natural_ref, jnp.concatenate(afters, axis=0))
    attn_ref[...] = shuffled(order_ref, jnp.concatenate(normals, axis=0))
    for copy in prefetch:
        copy.wait()


def convolve(shape, smalls, larges, project_weight, qkv_weight, out_weight):
    rows, cols = shape
    features = larges[-1]
    count, channels = features.shape
    width = larges[0].shape[1] * 2
    inputs = [*smalls, *larges]
    steps = width // WIDE
    around = smalls[0].shape[1]
    return pl.pallas_call(
        functools.partial(conv_kernel, shape),
        out_shape=like(features, features, qkv_weight, out_weight),
        in_specs=[INSIDE] * len(inputs) + [OUTSIDE] * 3,
        out_specs=[INSIDE] * 4,
        scratch_shapes=[
            pltpu.VMEM((around, channels), jnp.bfloat16),
            pltpu.VMEM((TWO, around, BLOCK), jnp.float32),
            pltpu.VMEM((WIDE // LANES, rows + 2, FOLD + 8, LANES), jnp.float32),
            pltpu.VMEM((WIDE // LANES, rows + 2, FOLD + 8, LANES), jnp.float32),
            pltpu.VMEM((2, count, WIDE), jnp.bfloat16),
            pltpu.VMEM((count, channels), jnp.float32),
            pltpu.VMEM((steps, WIDE, channels), jnp.bfloat16),
            pltpu.SemaphoreType.DMA((2,)),
            pltpu.SemaphoreType.DMA((steps,)),
        ],
        cost_estimate=pl.CostEstimate(
            flops=4 * count * channels * width,
            bytes_accessed=4 * channels * width,
            transcendentals=count * width,
        ),
        compiler_params=pltpu.CompilerParams(vmem_limit_bytes=24 << 20),
        name="depthwise_project",
    )(*inputs, in_hbm(project_weight), in_hbm(qkv_weight), in_hbm(out_weight))


def swap(cells, axis, count, odd_pairs):
    pairs = [(i, i + 1) for i in range(1 if odd_pairs else 0, count - 1, 2)]
    return lax.ppermute(cells, axis, pairs + [(j, i) for i, j in pairs])


def attend_kernel(
    group_size,
    x_ref,
    pick_ref,
    place_ref,
    qkv_weight_ref,
    qkv_bias_ref,
    out_weight_ref,
    out_bias_ref,
    o_ref,
    qkv_ref,
    mixed_ref,
    probs_ref,
):
    count, channels = x_ref.shape
    f32, bf16 = jnp.float32, jnp.bfloat16
    x = shuffled(pick_ref, x_ref[...])
    step = 256
    for lo in range(0, 3 * channels, step):
        cols = slice(lo, lo + step)
        part = jnp.dot(x, qkv_weight_ref[:, cols], preferred_element_type=f32)
        qkv_ref[:, cols] = (part + row_of(qkv_bias_ref, cols)).astype(bf16)

    wide = PACK * group_size
    lane = lax.broadcasted_iota(jnp.int32, (wide, LANES), 1) // HEAD_DIM
    row = lax.broadcasted_iota(jnp.int32, (wide, LANES), 0) // group_size
    own = (lane == row).astype(f32).astype(bf16)
    block_row = lax.broadcasted_iota(jnp.int32, (wide, wide), 0) // group_size
    block_col = lax.broadcasted_iota(jnp.int32, (wide, wide), 1) // group_size
    same = (block_row == block_col).astype(f32).astype(bf16)
    scale = math.log2(math.e) / math.sqrt(HEAD_DIM)
    top = float(jnp.finfo(bf16).max)
    chunks = channels // LANES

    def one_group(group, probs_ref):
        rows = pl.ds(pl.multiple_of(group * group_size, group_size), group_size)
        for chunk in range(chunks):
            lo = chunk * LANES
            query = qkv_ref[rows, lo : lo + LANES]
            key = qkv_ref[rows, channels + lo : channels + lo + LANES]
            keys = jnp.concatenate([key] * PACK, axis=0) * own
            scores = lax.dot_general(
                query, keys, (((1,), (1,)), ((), ())), preferred_element_type=f32
            )
            probs_ref[chunk * group_size : (chunk + 1) * group_size, :] = jnp.exp2(scores * scale)
        weights = probs_ref[...]
        total = jnp.dot(jnp.minimum(weights, top).astype(bf16), same, preferred_element_type=f32)
        probs = (weights / total).astype(bf16)
        for chunk in range(chunks):
            lo = chunk * LANES
            value = qkv_ref[rows, 2 * channels + lo : 2 * channels + lo + LANES]
            values = jnp.concatenate([value] * PACK, axis=0) * own
            mixed_ref[rows, lo : lo + LANES] = jnp.dot(
                probs[chunk * group_size : (chunk + 1) * group_size],
                values,
                preferred_element_type=f32,
            ).astype(bf16)

    together = probs_ref.shape[0]

    def some_groups(at, carry):
        for k in range(together):
            one_group(at * together + k, probs_ref.at[k])
        return carry

    lax.fori_loop(0, count // group_size // together, some_groups, 0)
    result = jnp.dot(mixed_ref[...], out_weight_ref[...], preferred_element_type=f32)
    o_ref[...] = shuffled(place_ref, (result + row_of(out_bias_ref)).astype(bf16))


def attend(tokens, pick, place, group_size, qkv_weight, qkv_bias, out_weight, out_bias):
    count, channels = tokens.shape
    arrays = [tokens, pick, place, qkv_weight, qkv_bias, out_weight, out_bias]
    return pl.pallas_call(
        functools.partial(attend_kernel, group_size),
        out_shape=jax.ShapeDtypeStruct((count, channels), jnp.bfloat16),
        in_specs=[INSIDE] * len(arrays),
        out_specs=INSIDE,
        scratch_shapes=[
            pltpu.VMEM((count, 3 * channels), jnp.bfloat16),
            pltpu.VMEM((count, channels), jnp.bfloat16),
            pltpu.VMEM(
                (TOGETHER, channels // LANES * group_size, PACK * group_size), jnp.float32
            ),
        ],
        cost_estimate=pl.CostEstimate(
            flops=10 * count * channels * channels, bytes_accessed=8 << 20, transcendentals=1 << 20
        ),
        compiler_params=pltpu.CompilerParams(vmem_limit_bytes=16 << 20),
        name="grid_attention",
    )(*arrays)


def per_device(
    features,
    norm_scale,
    norm_shift,
    expand_weight,
    expand_bias,
    depth_kernel,
    depth_bias,
    project_weight,
    project_bias,
    attn_gain,
    attn_shift,
    qkv_weight,
    qkv_bias,
    out_weight,
    out_bias,
):
    tile_rows, tile_cols, channels = features.shape
    row_count = lax.axis_size("row")
    col_count = lax.axis_size("col")
    row_at = lax.axis_index("row")
    flat = features.reshape(-1, channels)
    tall = tile_rows + 2
    strip = -(-tall // 16) * 16
    planes = tile_cols // FOLD
    one_row = np.arange(tile_cols).reshape(FOLD, planes).T.reshape(-1)
    fold = (np.arange(tile_rows)[:, None] * tile_cols + one_row[None]).reshape(-1)
    unfold = np.argsort(fold)
    columns = np.full((2, strip), -1)
    columns[0, 1 : tall - 1] = np.arange(tile_rows) * tile_cols
    columns[1, 1 : tall - 1] = np.arange(tile_rows) * tile_cols + tile_cols - 1

    def targets(sources, count):
        sources = np.asarray(sources).reshape(-1)
        found = np.full(count, -1, np.int32)
        found[sources[sources >= 0]] = np.flatnonzero(sources >= 0)
        return jnp.asarray(found)[None]

    count = tile_rows * tile_cols

    row_even = row_at % 2 == 0
    near = lax.dynamic_slice_in_dim(features, jnp.where(row_even, tile_rows - 1, 0), 1, 0)[0]
    far = lax.dynamic_slice_in_dim(features, jnp.where(row_even, 0, tile_rows - 1), 1, 0)[0]
    first_row = swap(near, "row", row_count, False)
    second_row = swap(far, "row", row_count, True)
    fold_row = max(1, GRID // row_count)
    fold_col = max(1, GRID // col_count)
    parity_row = max(1, row_count // GRID)
    parity_col = max(1, col_count // GRID)
    block_row = tile_rows // (fold_row * row_count)
    block_col = tile_cols // (fold_col * col_count)
    source = np.arange(tile_rows * tile_cols).reshape(
        fold_row, row_count, block_row, fold_col, col_count, block_col
    )
    source = source.transpose(1, 4, 0, 2, 3, 5).reshape(-1)
    around = np.concatenate(
        [one_row, tile_cols + one_row, 2 * tile_cols + np.arange(2 * strip)]
    )
    layout = np.arange(tile_rows * tile_cols).reshape(
        row_count // parity_row,
        parity_row,
        col_count // parity_col,
        parity_col,
        fold_row,
        block_row,
        fold_col,
        block_col,
    )
    pick = layout.transpose(1, 3, 5, 7, 0, 2, 4, 6)
    group_size = math.prod(pick.shape[4:])
    pick = pick.reshape(-1)
    low, folded, edges, low_weight, *smalls = expand_low(
        targets(fold, count),
        targets(columns, count),
        2 * strip,
        flat,
        expand_weight,
        [
            norm_scale,
            norm_shift,
            expand_bias,
            targets(around, around.size),
            targets(unfold, count),
            targets(unfold[source], count),
            depth_kernel,
            depth_bias,
            project_bias,
            attn_gain,
            attn_shift,
            targets(pick, count),
            targets(np.argsort(pick), count),
            qkv_bias,
            out_bias,
        ],
    )
    scale, shift, bias = smalls[:3]
    first_col, second_col = edges_to_send(tall, first_row, second_row, edges)
    high, high_weight = expand_high(folded, first_col, scale, shift, expand_weight, bias)
    first_col = swap(first_col, "col", col_count, False)
    second_col = swap(second_col, "col", col_count, True)
    after_conv, ordered, qkv_weight, out_weight = convolve(
        (tile_rows, tile_cols),
        [*smalls[3:5], smalls[5], scale, shift, bias, *smalls[6:11]],
        [
            low,
            high,
            first_row,
            second_row,
            first_col,
            second_col,
            low_weight,
            high_weight,
            folded,
        ],
        project_weight,
        qkv_weight,
        out_weight,
    )
    pick, place, qkv_bias, out_bias = smalls[11:]
    after_conv = after_conv.reshape(features.shape)
    ordered = ordered.reshape(
        row_count * col_count, fold_row, block_row, fold_col, block_col, channels
    )
    received = lax.all_to_all(ordered, ("row", "col"), split_axis=0, concat_axis=0, tiled=True)
    tokens = received.reshape(-1, channels)
    answered = attend(
        tokens, pick, place, group_size, qkv_weight, qkv_bias, out_weight, out_bias
    ).reshape(received.shape)
    returned = lax.all_to_all(answered, ("row", "col"), split_axis=0, concat_axis=0, tiled=True)
    returned_tiles = returned.reshape(
        row_count, col_count, fold_row, block_row, fold_col, block_col, channels
    ).transpose(2, 0, 3, 4, 1, 5, 6)
    attended = returned_tiles.reshape(tile_rows, tile_cols, channels)
    return (after_conv.astype(jnp.float32) + attended.astype(jnp.float32)).astype(jnp.bfloat16)


def solution(mesh):
    return jax.shard_map(
        per_device,
        mesh=mesh,
        in_specs=(P("row", "col", None),) + (P(),) * 14,
        out_specs=P("row", "col", None),
        check_vma=False,
    )
```

```python
import functools
import math

import jax
import jax.numpy as jnp
import numpy as np
from jax import lax
from jax.experimental import pallas as pl
from jax.experimental.pallas import tpu as pltpu
from jax.sharding import PartitionSpec as P

HEAD_DIM = 32
GRID = 8
LANES = 128
PACK = LANES // HEAD_DIM
TOGETHER = 8


def gelu(v):
    half = 0.5 * v
    inner = v * (0.7978845608028654 + 0.035677408136300125 * (v * v))
    return half + half * jnp.tanh(inner)


def in_hbm(array):
    return pltpu.with_memory_space_constraint(array, pltpu.HBM)


def row_of(ref, cols=slice(None)):
    return ref[cols].reshape(1, -1)


def fetch(source, target, sems, start, count):
    block = target.shape[-1]
    return [
        pltpu.make_async_copy(
            source.at[:, pl.ds((start + i) * block, block)], target.at[i], sems.at[i]
        )
        for i in range(count)
    ]


FOLD = 8


def shuffled(target_ref, values, count=None):
    shape = (count or values.shape[0], values.shape[0])
    row = lax.broadcasted_iota(jnp.int32, shape, 0)
    pick = (row == target_ref[...]).astype(jnp.float32).astype(jnp.bfloat16)
    return jnp.dot(pick, values, preferred_element_type=jnp.float32).astype(jnp.bfloat16)


OUTSIDE = pl.BlockSpec(memory_space=pltpu.HBM)


INSIDE = pl.BlockSpec(memory_space=pltpu.VMEM)
BLOCK = 256
TWO = 2
WIDE = TWO * BLOCK
TALL = 256


def like(*arrays):
    return [jax.ShapeDtypeStruct(array.shape, array.dtype) for array in arrays]


def expand_all(start, normed_ref, bias_ref, copies, held_ref, o_ref, later=()):
    steps, _, block = held_ref.shape
    count = normed_ref.shape[0]
    for i in range(steps):
        if copies:
            copies[i].wait()
        if i == 0:
            for copy in later:
                copy.start()
        cols = slice(i * block, (i + 1) * block)
        bias = row_of(bias_ref, slice((start + i) * block, (start + i + 1) * block))
        for lo in range(0, count, TALL):
            rows = slice(lo, lo + TALL)
            part = jnp.dot(normed_ref[rows], held_ref[i], preferred_element_type=jnp.float32)
            o_ref[rows, cols] = gelu(part + bias)


def normalize(x, scale_ref, shift_ref):
    return (x.astype(jnp.float32) * row_of(scale_ref) + row_of(shift_ref)).astype(jnp.bfloat16)


def load_kernel(row_size, *refs):
    x_ref, *refs = refs
    count = (len(refs) - 4) // 2
    sources, (far_ref, near_ref, x_held_ref, *targets, sems) = refs[:count], refs[count:]
    height = x_ref.shape[0] // row_size
    even = lax.rem(lax.axis_index("row"), 2) == 0
    pairs = [
        (x_ref.at[pl.ds(pl.multiple_of(at * row_size, row_size), row_size)], target)
        for at, target in (
            (jnp.where(even, 0, height - 1), far_ref),
            (jnp.where(even, height - 1, 0), near_ref),
        )
    ]
    pairs += [(x_ref, x_held_ref), *zip(sources, targets, strict=True)]
    copies = [
        pltpu.make_async_copy(source, target, sems.at[i])
        for i, (source, target) in enumerate(pairs)
    ]
    for copy in copies:
        copy.start()
    for copy in copies:
        copy.wait()


def load(row_size, tokens, *smalls):
    row = jax.ShapeDtypeStruct((row_size, tokens.shape[1]), tokens.dtype)
    shapes = [row, row, *like(tokens, *smalls)]
    return pl.pallas_call(
        functools.partial(load_kernel, row_size),
        out_shape=shapes,
        in_specs=[OUTSIDE] * (1 + len(smalls)),
        out_specs=[INSIDE] * len(shapes),
        scratch_shapes=[pltpu.SemaphoreType.DMA((len(shapes),))],
        compiler_params=pltpu.CompilerParams(vmem_limit_bytes=1 << 20),
        name="load",
    )(*[in_hbm(array) for array in (tokens, *smalls)])


def expand_low_kernel(smalls, *refs):
    x_ref, fold_ref, columns_ref, scale_ref, shift_ref, bias_ref, weight_ref, *refs = refs
    sources, refs = refs[:smalls], refs[smalls:]
    o_ref, folded_ref, edges_ref, held_ref, high_held_ref, *refs = refs
    targets, (normed_ref, sems, high_sems, small_sems) = refs[:smalls], refs[smalls:]
    hand_on = [
        pltpu.make_async_copy(source, target, small_sems.at[i])
        for i, (source, target) in enumerate(zip(sources, targets, strict=True))
    ]
    steps = held_ref.shape[0]
    copies = fetch(weight_ref, held_ref, sems, 0, steps)
    later = hand_on + fetch(weight_ref, high_held_ref, high_sems, steps, steps)
    for copy in copies:
        copy.start()
    x = x_ref[...]
    folded = shuffled(fold_ref, x)
    folded_ref[...] = folded
    edges_ref[...] = shuffled(columns_ref, x, edges_ref.shape[0])
    normed_ref[...] = normalize(folded, scale_ref, shift_ref)
    expand_all(0, normed_ref, bias_ref, copies, held_ref, o_ref, later)
    for copy in later:
        copy.wait()


def expand_high_kernel(scale_ref, shift_ref, bias_ref, folded_ref, held_ref, _, o_ref, normed_ref):
    normed_ref[...] = normalize(folded_ref[...], scale_ref, shift_ref)
    expand_all(held_ref.shape[0], normed_ref, bias_ref, (), held_ref, o_ref)


def expand_low(held, edge_count, weight, smalls):
    count, channels = held[0].shape
    width = weight.shape[1] // 2
    steps = width // BLOCK
    shapes = [
        jax.ShapeDtypeStruct((count, width), jnp.float32),
        jax.ShapeDtypeStruct((count, channels), jnp.bfloat16),
        jax.ShapeDtypeStruct((edge_count, channels), jnp.bfloat16),
        *[jax.ShapeDtypeStruct((steps, channels, BLOCK), jnp.bfloat16)] * 2,
        *like(*smalls),
    ]
    return pl.pallas_call(
        functools.partial(expand_low_kernel, len(smalls)),
        out_shape=shapes,
        in_specs=[INSIDE] * len(held) + [OUTSIDE] * (1 + len(smalls)),
        out_specs=[INSIDE] * len(shapes),
        scratch_shapes=[
            pltpu.VMEM((count, channels), jnp.bfloat16),
            pltpu.SemaphoreType.DMA((steps,)),
            pltpu.SemaphoreType.DMA((steps,)),
            pltpu.SemaphoreType.DMA((len(smalls),)),
        ],
        cost_estimate=pl.CostEstimate(
            flops=2 * count * channels * width,
            bytes_accessed=2 * channels * width,
            transcendentals=count * width,
        ),
        compiler_params=pltpu.CompilerParams(vmem_limit_bytes=12 << 20),
        name="expand_low",
    )(*held, *[in_hbm(array) for array in (weight, *smalls)])


def expand_high(folded, after, scale, shift, held, bias):
    count, channels = folded.shape
    width = held.shape[0] * BLOCK
    return pl.pallas_call(
        expand_high_kernel,
        out_shape=jax.ShapeDtypeStruct((count, width), jnp.float32),
        in_specs=[INSIDE] * 5 + [pl.BlockSpec(memory_space=pl.ANY)],
        out_specs=INSIDE,
        scratch_shapes=[pltpu.VMEM((count, channels), jnp.bfloat16)],
        cost_estimate=pl.CostEstimate(
            flops=2 * count * channels * width,
            bytes_accessed=6 * channels * width,
            transcendentals=count * width,
        ),
        compiler_params=pltpu.CompilerParams(vmem_limit_bytes=12 << 20),
        name="expand_high",
    )(scale, shift, bias, folded, held, after)


def edges_kernel(tall, first_row_ref, second_row_ref, edges_ref, first_ref, second_ref):
    f32 = jnp.float32
    row_even = lax.rem(lax.axis_index("row"), 2) == 0
    col_even = lax.rem(lax.axis_index("col"), 2) == 0
    strip = first_ref.shape[0]
    last = first_row_ref.shape[0]
    spot = lax.broadcasted_iota(jnp.int32, (strip, 1), 0)

    def column(side, at):
        first = first_row_ref[at : at + 1].astype(f32)
        second = second_row_ref[at : at + 1].astype(f32)
        top = jnp.where(row_even, second, first)
        bottom = jnp.where(row_even, first, second)
        middle = edges_ref[side * strip : (side + 1) * strip].astype(f32)
        return jnp.where(spot == 0, top, jnp.where(spot == tall - 1, bottom, middle))

    left, right = column(0, 0), column(1, last - 1)
    first_ref[...] = jnp.where(col_even, right, left).astype(jnp.bfloat16)
    second_ref[...] = jnp.where(col_even, left, right).astype(jnp.bfloat16)


def edges_to_send(tall, first_row, second_row, edges):
    shape = jax.ShapeDtypeStruct((edges.shape[0] // 2, edges.shape[1]), edges.dtype)
    return pl.pallas_call(
        functools.partial(edges_kernel, tall),
        out_shape=[shape, shape],
        in_specs=[INSIDE] * 3,
        out_specs=[INSIDE] * 2,
        compiler_params=pltpu.CompilerParams(vmem_limit_bytes=2 << 20),
        name="edges",
    )(first_row, second_row, edges)


def conv_kernel(
    shape,
    halo_order_ref,
    natural_ref,
    order_ref,
    scale_ref,
    shift_ref,
    expand_bias_ref,
    depth_kernel_ref,
    depth_bias_ref,
    project_bias_ref,
    gain_ref,
    offset_ref,
    low_ref,
    high_ref,
    first_row_ref,
    second_row_ref,
    first_col_ref,
    second_col_ref,
    low_weight_ref,
    high_weight_ref,
    features_ref,
    project_weight_ref,
    qkv_weight_ref,
    out_weight_ref,
    after_ref,
    attn_ref,
    qkv_held_ref,
    out_held_ref,
    normed_ref,
    halo_hidden_ref,
    left_ref,
    right_ref,
    depth_ref,
    total_ref,
    project_held_ref,
    sems,
    project_sems,
):
    f32, bf16 = jnp.float32, jnp.bfloat16
    rows, cols = shape
    planes = cols // FOLD
    tall = rows + 2
    strip = first_col_ref.shape[0]
    prefetch = [
        pltpu.make_async_copy(qkv_weight_ref, qkv_held_ref, sems.at[0]),
        pltpu.make_async_copy(out_weight_ref, out_held_ref, sems.at[1]),
    ]
    half = low_weight_ref.shape[0] // TWO

    def project_copy(step):
        rows_at = pl.ds(pl.multiple_of(step * WIDE, WIDE), WIDE)
        return pltpu.make_async_copy(
            project_weight_ref.at[rows_at], project_held_ref.at[step], project_sems.at[step]
        )

    last = 2 * half - 1
    for step in range(last):
        project_copy(step).start()

    row_at, col_at = lax.axis_index("row"), lax.axis_index("col")
    row_even, col_even = lax.rem(row_at, 2) == 0, lax.rem(col_at, 2) == 0
    has_top = (row_at > 0).astype(f32)
    has_bottom = (row_at < lax.axis_size("row") - 1).astype(f32)
    has_left = (col_at > 0).astype(f32)
    has_right = (col_at < lax.axis_size("col") - 1).astype(f32)
    top_at = jnp.where(row_even, cols, 0)
    bottom_at = jnp.where(row_even, 0, cols)
    left_at = 2 * cols + jnp.where(col_even, strip, 0)
    right_at = 2 * cols + jnp.where(col_even, 0, strip)
    spot = lax.broadcasted_iota(jnp.int32, (2 * cols + 2 * strip, 1), 0)
    first_there = jnp.where(row_even, has_bottom, has_top)
    second_there = jnp.where(row_even, has_top, has_bottom)
    near_there = jnp.where(col_even, has_right, has_left)
    far_there = jnp.where(col_even, has_left, has_right)
    place = lax.rem(spot, strip)
    ends = jnp.where(place == 0, has_top, jnp.where(place == tall - 1, has_bottom, 1.0))
    keep = jnp.where(
        spot < cols,
        first_there,
        jnp.where(
            spot < 2 * cols,
            second_there,
            ends * jnp.where(spot < 2 * cols + strip, near_there, far_there),
        ),
    )

    halo = jnp.concatenate(
        [first_row_ref[...], second_row_ref[...], first_col_ref[...], second_col_ref[...]], axis=0
    )
    normed_ref[...] = shuffled(halo_order_ref, normalize(halo, scale_ref, shift_ref))

    depth_ref[1] = jnp.zeros_like(depth_ref[1])
    project_held_ref[last] = jnp.zeros_like(project_held_ref[last])
    total_ref[...] = features_ref[...].astype(f32) + row_of(project_bias_ref)

    def add_chunk(at, slot):
        total_ref[...] += jnp.dot(
            depth_ref[slot], project_held_ref[at], preferred_element_type=f32
        )

    def convolve(step, hidden_ref, weight_ref, offset):
        slot = lax.rem(step + offset, 2)
        at = step + offset

        @pl.when(at > 0)
        def _():
            project_copy(at - 1).wait()

        add_chunk(jnp.where(at > 0, at - 1, last), 1 - slot)
        for sub in range(TWO):
            convolve_block(step * TWO + sub, hidden_ref, weight_ref, offset * TWO, slot, sub)

    def convolve_block(step, hidden_ref, weight_ref, offset, slot, sub):
        base = pl.multiple_of((step + offset) * BLOCK, BLOCK)
        part = jnp.dot(normed_ref[...], weight_ref[step], preferred_element_type=f32)
        bias = expand_bias_ref[pl.ds(base, BLOCK)].reshape(1, BLOCK)
        halo_hidden_ref[sub] = gelu(part + bias) * keep
        for lane in range(BLOCK // LANES):
            lanes = slice(lane * LANES, (lane + 1) * LANES)
            wide_lanes = slice(sub * BLOCK + lane * LANES, sub * BLOCK + (lane + 1) * LANES)
            inner = pl.ds(pl.multiple_of(step * BLOCK + lane * LANES, LANES), LANES)
            outer = pl.ds(pl.multiple_of(base + lane * LANES, LANES), LANES)
            left = halo_hidden_ref[sub, pl.ds(pl.multiple_of(left_at, 8), strip), lanes]
            right = halo_hidden_ref[sub, pl.ds(pl.multiple_of(right_at, 8), strip), lanes]

            def cell(r, j):
                if r == 0 or r == tall - 1:
                    at = (top_at if r == 0 else bottom_at) + j * FOLD
                    return halo_hidden_ref[sub, pl.ds(pl.multiple_of(at, 8), FOLD), lanes]
                at = ((r - 1) * planes + j) * FOLD
                return hidden_ref[at : at + FOLD, inner]

            for r in range(tall):
                left_ref[BLOCK // LANES * sub + lane, r, 8 : 8 + FOLD, :] = cell(r, planes - 1)
                left_ref[BLOCK // LANES * sub + lane, r, 7:8, :] = left[r : r + 1]
                right_ref[BLOCK // LANES * sub + lane, r, 0:FOLD, :] = cell(r, 0)
                right_ref[BLOCK // LANES * sub + lane, r, FOLD : FOLD + 1, :] = right[r : r + 1]

            def shifted(r, j):
                if j < 0:
                    return left_ref[BLOCK // LANES * sub + lane, r, 7 : 7 + FOLD, :]
                if j == planes:
                    return right_ref[BLOCK // LANES * sub + lane, r, 1 : 1 + FOLD, :]
                return cell(r, j)

            taps = [
                [
                    jnp.broadcast_to(depth_kernel_ref[a, b : b + 1, outer], (FOLD, LANES))
                    for b in range(3)
                ]
                for a in range(3)
            ]
            bias = jnp.broadcast_to(depth_bias_ref[outer].reshape(1, LANES), (FOLD, LANES))
            pair = 2
            for start in range(0, planes, pair):
                sums = [[None] * rows for _ in range(pair)]
                for r in range(tall):
                    near = [shifted(r, start - 1 + b) for b in range(pair + 2)]
                    for k in range(pair):
                        for a in range(3):
                            h = r - a
                            if 0 <= h < rows:
                                line = near[k] * taps[a][0] + near[k + 1] * taps[a][1]
                                line = line + near[k + 2] * taps[a][2]
                                old = sums[k][h]
                                sums[k][h] = line + (bias if old is None else old)
                    h = r - 2
                    if h >= 0:
                        lo = (h * planes + start) * FOLD
                        depth_ref[slot, lo : lo + pair * FOLD, wide_lanes] = jnp.concatenate(
                            [gelu(sums[k][h]) for k in range(pair)], axis=0
                        ).astype(bf16)

    def low_step(step, carry):
        convolve(step, low_ref, low_weight_ref, 0)
        return carry

    def high_step(step, carry):
        convolve(step, high_ref, high_weight_ref, half)
        return carry

    lax.fori_loop(0, half, low_step, 0)
    project_copy(last).start()
    for copy in prefetch:
        copy.start()
    lax.fori_loop(0, half, high_step, 0)
    project_copy(last).wait()

    group = 256
    normals, afters = [], []
    for lo in range(0, rows * cols, group):
        part = slice(lo, lo + group)
        total = total_ref[part] + jnp.dot(
            depth_ref[last % 2, part], project_held_ref[last], preferred_element_type=f32
        )
        after = total.astype(bf16)
        wide = after.astype(f32)
        center = wide - jnp.mean(wide, axis=-1, keepdims=True)
        spread = jnp.mean(center * center, axis=-1, keepdims=True)
        normal = center * lax.rsqrt(spread + 1e-06) * row_of(gain_ref) + row_of(offset_ref)
        afters.append(after)
        normals.append(normal.astype(bf16))
    after_ref[...] = shuffled(natural_ref, jnp.concatenate(afters, axis=0))
    attn_ref[...] = shuffled(order_ref, jnp.concatenate(normals, axis=0))
    for copy in prefetch:
        copy.wait()


def convolve(shape, smalls, larges, project_weight, qkv_weight, out_weight):
    rows, _ = shape
    features = larges[-1]
    count, channels = features.shape
    width = larges[0].shape[1] * 2
    inputs = [*smalls, *larges]
    steps = width // WIDE
    around = smalls[0].shape[1]
    return pl.pallas_call(
        functools.partial(conv_kernel, shape),
        out_shape=like(features, features, qkv_weight, out_weight),
        in_specs=[INSIDE] * len(inputs) + [OUTSIDE] * 3,
        out_specs=[INSIDE] * 4,
        scratch_shapes=[
            pltpu.VMEM((around, channels), jnp.bfloat16),
            pltpu.VMEM((TWO, around, BLOCK), jnp.float32),
            pltpu.VMEM((WIDE // LANES, rows + 2, FOLD + 8, LANES), jnp.float32),
            pltpu.VMEM((WIDE // LANES, rows + 2, FOLD + 8, LANES), jnp.float32),
            pltpu.VMEM((2, count, WIDE), jnp.bfloat16),
            pltpu.VMEM((count, channels), jnp.float32),
            pltpu.VMEM((steps, WIDE, channels), jnp.bfloat16),
            pltpu.SemaphoreType.DMA((2,)),
            pltpu.SemaphoreType.DMA((steps,)),
        ],
        cost_estimate=pl.CostEstimate(
            flops=4 * count * channels * width,
            bytes_accessed=4 * channels * width,
            transcendentals=count * width,
        ),
        compiler_params=pltpu.CompilerParams(vmem_limit_bytes=24 << 20),
        name="depthwise_project",
    )(*inputs, in_hbm(project_weight), in_hbm(qkv_weight), in_hbm(out_weight))


def swap(cells, axis, count, odd_pairs):
    pairs = [(i, i + 1) for i in range(1 if odd_pairs else 0, count - 1, 2)]
    return lax.ppermute(cells, axis, pairs + [(j, i) for i, j in pairs])


def attend_kernel(
    group_size,
    x_ref,
    pick_ref,
    place_ref,
    qkv_weight_ref,
    qkv_bias_ref,
    out_weight_ref,
    out_bias_ref,
    o_ref,
    qkv_ref,
    mixed_ref,
    probs_ref,
):
    count, channels = x_ref.shape
    f32, bf16 = jnp.float32, jnp.bfloat16
    x = shuffled(pick_ref, x_ref[...])
    step = 256
    for lo in range(0, 3 * channels, step):
        cols = slice(lo, lo + step)
        part = jnp.dot(x, qkv_weight_ref[:, cols], preferred_element_type=f32)
        qkv_ref[:, cols] = (part + row_of(qkv_bias_ref, cols)).astype(bf16)

    wide = PACK * group_size
    lane = lax.broadcasted_iota(jnp.int32, (wide, LANES), 1) // HEAD_DIM
    row = lax.broadcasted_iota(jnp.int32, (wide, LANES), 0) // group_size
    own = (lane == row).astype(f32).astype(bf16)
    block_row = lax.broadcasted_iota(jnp.int32, (wide, wide), 0) // group_size
    block_col = lax.broadcasted_iota(jnp.int32, (wide, wide), 1) // group_size
    same = (block_row == block_col).astype(f32).astype(bf16)
    scale = math.log2(math.e) / math.sqrt(HEAD_DIM)
    top = float(jnp.finfo(bf16).max)
    chunks = channels // LANES

    def one_group(group, probs_ref):
        rows = pl.ds(pl.multiple_of(group * group_size, group_size), group_size)
        for chunk in range(chunks):
            lo = chunk * LANES
            query = qkv_ref[rows, lo : lo + LANES]
            key = qkv_ref[rows, channels + lo : channels + lo + LANES]
            keys = jnp.concatenate([key] * PACK, axis=0) * own
            scores = lax.dot_general(
                query, keys, (((1,), (1,)), ((), ())), preferred_element_type=f32
            )
            probs_ref[chunk * group_size : (chunk + 1) * group_size, :] = jnp.exp2(scores * scale)
        weights = probs_ref[...]
        total = jnp.dot(jnp.minimum(weights, top).astype(bf16), same, preferred_element_type=f32)
        probs = (weights / total).astype(bf16)
        for chunk in range(chunks):
            lo = chunk * LANES
            value = qkv_ref[rows, 2 * channels + lo : 2 * channels + lo + LANES]
            values = jnp.concatenate([value] * PACK, axis=0) * own
            mixed_ref[rows, lo : lo + LANES] = jnp.dot(
                probs[chunk * group_size : (chunk + 1) * group_size],
                values,
                preferred_element_type=f32,
            ).astype(bf16)

    together = probs_ref.shape[0]

    def some_groups(at, carry):
        for k in range(together):
            one_group(at * together + k, probs_ref.at[k])
        return carry

    lax.fori_loop(0, count // group_size // together, some_groups, 0)
    result = jnp.dot(mixed_ref[...], out_weight_ref[...], preferred_element_type=f32)
    o_ref[...] = shuffled(place_ref, (result + row_of(out_bias_ref)).astype(bf16))


def attend(tokens, pick, place, group_size, qkv_weight, qkv_bias, out_weight, out_bias):
    count, channels = tokens.shape
    arrays = [tokens, pick, place, qkv_weight, qkv_bias, out_weight, out_bias]
    return pl.pallas_call(
        functools.partial(attend_kernel, group_size),
        out_shape=jax.ShapeDtypeStruct((count, channels), jnp.bfloat16),
        in_specs=[INSIDE] * len(arrays),
        out_specs=INSIDE,
        scratch_shapes=[
            pltpu.VMEM((count, 3 * channels), jnp.bfloat16),
            pltpu.VMEM((count, channels), jnp.bfloat16),
            pltpu.VMEM(
                (TOGETHER, channels // LANES * group_size, PACK * group_size), jnp.float32
            ),
        ],
        cost_estimate=pl.CostEstimate(
            flops=10 * count * channels * channels, bytes_accessed=8 << 20, transcendentals=1 << 20
        ),
        compiler_params=pltpu.CompilerParams(vmem_limit_bytes=16 << 20),
        name="grid_attention",
    )(*arrays)


def per_device(
    features,
    norm_scale,
    norm_shift,
    expand_weight,
    expand_bias,
    depth_kernel,
    depth_bias,
    project_weight,
    project_bias,
    attn_gain,
    attn_shift,
    qkv_weight,
    qkv_bias,
    out_weight,
    out_bias,
):
    tile_rows, tile_cols, channels = features.shape
    row_count = lax.axis_size("row")
    col_count = lax.axis_size("col")
    flat = features.reshape(-1, channels)
    tall = tile_rows + 2
    strip = -(-tall // 16) * 16
    planes = tile_cols // FOLD
    one_row = np.arange(tile_cols).reshape(FOLD, planes).T.reshape(-1)
    fold = (np.arange(tile_rows)[:, None] * tile_cols + one_row[None]).reshape(-1)
    unfold = np.argsort(fold)
    columns = np.full((2, strip), -1)
    columns[0, 1 : tall - 1] = np.arange(tile_rows) * tile_cols
    columns[1, 1 : tall - 1] = np.arange(tile_rows) * tile_cols + tile_cols - 1

    def targets(sources, count):
        sources = np.asarray(sources).reshape(-1)
        found = np.full(count, -1, np.int32)
        found[sources[sources >= 0]] = np.flatnonzero(sources >= 0)
        return jnp.asarray(found)[None]

    count = tile_rows * tile_cols

    far, near, *held = load(
        tile_cols,
        flat,
        targets(fold, count),
        targets(columns, count),
        norm_scale,
        norm_shift,
        expand_bias,
    )
    second_row = swap(far, "row", row_count, True)
    first_row = swap(near, "row", row_count, False)
    fold_row = max(1, GRID // row_count)
    fold_col = max(1, GRID // col_count)
    parity_row = max(1, row_count // GRID)
    parity_col = max(1, col_count // GRID)
    block_row = tile_rows // (fold_row * row_count)
    block_col = tile_cols // (fold_col * col_count)
    source = np.arange(tile_rows * tile_cols).reshape(
        fold_row, row_count, block_row, fold_col, col_count, block_col
    )
    source = source.transpose(1, 4, 0, 2, 3, 5).reshape(-1)
    around = np.concatenate(
        [one_row, tile_cols + one_row, 2 * tile_cols + np.arange(2 * strip)]
    )
    layout = np.arange(tile_rows * tile_cols).reshape(
        row_count // parity_row,
        parity_row,
        col_count // parity_col,
        parity_col,
        fold_row,
        block_row,
        fold_col,
        block_col,
    )
    pick = layout.transpose(1, 3, 5, 7, 0, 2, 4, 6)
    group_size = math.prod(pick.shape[4:])
    pick = pick.reshape(-1)
    low, folded, edges, low_weight, high_weight, *smalls = expand_low(
        held,
        2 * strip,
        expand_weight,
        [
            targets(around, around.size),
            targets(unfold, count),
            targets(unfold[source], count),
            depth_kernel,
            depth_bias,
            project_bias,
            attn_gain,
            attn_shift,
            targets(pick, count),
            targets(np.argsort(pick), count),
            qkv_bias,
            out_bias,
        ],
    )
    scale, shift, bias = held[3:]
    first_col, second_col = edges_to_send(tall, first_row, second_row, edges)
    high = expand_high(folded, first_col, scale, shift, high_weight, bias)
    first_col = swap(first_col, "col", col_count, False)
    second_col = swap(second_col, "col", col_count, True)
    after_conv, ordered, qkv_weight, out_weight = convolve(
        (tile_rows, tile_cols),
        [*smalls[:3], scale, shift, bias, *smalls[3:8]],
        [
            low,
            high,
            first_row,
            second_row,
            first_col,
            second_col,
            low_weight,
            high_weight,
            folded,
        ],
        project_weight,
        qkv_weight,
        out_weight,
    )
    pick, place, qkv_bias, out_bias = smalls[8:]
    after_conv = after_conv.reshape(features.shape)
    ordered = ordered.reshape(
        row_count * col_count, fold_row, block_row, fold_col, block_col, channels
    )
    received = lax.all_to_all(ordered, ("row", "col"), split_axis=0, concat_axis=0, tiled=True)
    tokens = received.reshape(-1, channels)
    answered = attend(
        tokens, pick, place, group_size, qkv_weight, qkv_bias, out_weight, out_bias
    ).reshape(received.shape)
    returned = lax.all_to_all(answered, ("row", "col"), split_axis=0, concat_axis=0, tiled=True)
    returned_tiles = returned.reshape(
        row_count, col_count, fold_row, block_row, fold_col, block_col, channels
    ).transpose(2, 0, 3, 4, 1, 5, 6)
    attended = returned_tiles.reshape(tile_rows, tile_cols, channels)
    return (after_conv.astype(jnp.float32) + attended.astype(jnp.float32)).astype(jnp.bfloat16)


def solution(mesh):
    return jax.shard_map(
        per_device,
        mesh=mesh,
        in_specs=(P("row", "col", None),) + (P(),) * 14,
        out_specs=P("row", "col", None),
        check_vma=False,
    )
```
